32 devices in a mesh: ent: 16 (over z, y, x), grp: 2 (over core).
Axes of the slice: x: 2, y: 2, z: 4, core: 2. Of those that a mesh axis runs over, the one named last changes fastest.
Arguments:
- entity_table: bfloat16 [8192, 1024], P('ent'), may hold values from -2.5 to 2.5
- rel_phases: float32 [822, 512], replicated, may hold values from -3.1416 to 3.1416
- head_ids: int32 [8192], P(('ent', 'grp')), may hold values from 0 to 511
- rel_ids: int32 [8192], P(('ent', 'grp')), may hold values from 0 to 821
- target_pos: int32 [8192], P(('ent', 'grp')), may hold values from 0 to 511
- block_owner: int32 [4], replicated, may hold values from 0 to 15
- block_local: int32 [4], replicated, may hold values from 0 to 3
Outputs:
- losses: float32 [8192], P(('ent', 'grp'))
- head_grad: bfloat16 [8192, 1024], P(('ent', 'grp'))
- table_grad: bfloat16 [8192, 1024], P('ent')
- rel_grad: float32 [822, 512], replicated
The draws below stay inside these ranges and needn't reach their ends.
Inputs may be any that keep to these rules, and one draw needn't show every extreme that they name: query q on device d (ent then grp) has head row (d // 2) * 512 + head_ids[q]. `target_pos`: position among the 512 candidates, block after block. Block b covers table rows from (block_owner[b] * 4 + block_local[b]) * 128 on; blocks may repeat.
All inputs are finite; a program needn't handle non-finite values.
Results may differ from the reference program's by a relative error of at most 0.0057.
Values may be sent and summed in bfloat16 or wider, within the bound.
A program may use at most 64 MiB of HBM per device.

```python
import math
import jax
import jax.numpy as jnp
import numpy as np
from jax import lax

K = 512
R = 822
BLK = 128
NBLK = 4
ENT_DEV = 512
Q_DEV = 256
SHARDS = 16
NENT = 8192
QUERIES = 8192
CAND = 512
N_ENT = 16
N_GRP = 2


def draw_entity_table(key, part):
    key_noise = jax.random.fold_in(key, 2)
    values = jnp.clip(0.25 * jax.random.normal(key_noise, (NENT, 2 * K), jnp.float32), -1.5, 1.5)
    return values.astype(jnp.bfloat16)


def draw_rel_phases(key, part):
    return jax.random.uniform(key, (R, K), jnp.float32, -3.1415, 3.1415)


def plant(values, rng, least, high):
    longest = values.shape.index(max(values.shape))
    spots = []
    for shift in (0, 1):
        where = [jax.random.randint(jax.random.fold_in(rng, axis), (), 0, length) for axis, length in enumerate(values.shape)]
        where[longest] = (where[longest] + shift) % values.shape[longest]
        spots.append(tuple(where))
    return values.at[spots[0]].set(least).at[spots[1]].set(high)


def cumulative_ranks(amount, slope):
    portions = [(1 << 20) // math.isqrt(grade ** slope) + 1 for grade in range(1, amount + 1)]
    width = 1 + sum(portions) // (1 << 30)
    return np.cumsum(np.array([max(1, weight // width) for weight in portions]))


def ranked(key, extent, number_of, lean):
    listing = cumulative_ranks(number_of, lean)
    ticket = jax.random.randint(jax.random.fold_in(key, 1), extent, 0, int(listing[number_of - 1]))
    rank = jnp.searchsorted(jnp.asarray(listing, jnp.int32), ticket, side="right")
    return jax.random.permutation(jax.random.fold_in(key, 2), number_of)[rank].astype(jnp.int32)


def setup_inputs(seed: int = 0) -> dict:
    arg_keys = jax.random.split(jax.random.key(seed), 8)
    return {
        "entity_table": draw_entity_table(jax.random.fold_in(arg_keys[7], 71), 0),
        "rel_phases": draw_rel_phases(jax.random.fold_in(arg_keys[7], 71), 0),
        "head_ids": plant(jax.random.randint(arg_keys[2], (QUERIES,), 0, ENT_DEV), jax.random.fold_in(arg_keys[2], 1), 0, ENT_DEV - 1).astype(jnp.int32),
        "rel_ids": plant(ranked(arg_keys[3], (QUERIES,), R, 2), jax.random.fold_in(arg_keys[3], 3), 0, R - 1).astype(jnp.int32),
        "target_pos": plant(jax.random.randint(arg_keys[4], (QUERIES,), 0, CAND), jax.random.fold_in(arg_keys[4], 1), 0, CAND - 1).astype(jnp.int32),
        "block_owner": plant(jax.random.randint(arg_keys[5], (NBLK,), 0, SHARDS), jax.random.fold_in(arg_keys[5], 1), 0, SHARDS - 1).astype(jnp.int32),
        "block_local": plant(jax.random.randint(arg_keys[6], (NBLK,), 0, ENT_DEV // BLK), jax.random.fold_in(arg_keys[6], 1), 0, (ENT_DEV // BLK) - 1).astype(jnp.int32),
    }


SOFTMAX_TEMPER = 2.0


def device_terms(heads, angles, targets, candidate_block, candidate_norm):
    half_dim = angles.shape[1]
    real_head = heads[:, :half_dim]
    imag_head = heads[:, half_dim:]
    cosine = jnp.cos(angles)
    sine = jnp.sin(angles)
    real_query = real_head * cosine - imag_head * sine
    imag_query = real_head * sine + imag_head * cosine
    query_reduced_precision = jnp.concatenate([real_query, imag_query], axis=1).astype(jnp.bfloat16)
    query_reduced_precision = lax.optimization_barrier(query_reduced_precision).astype(jnp.float32)
    logit_scores = (2.0 * jnp.dot(query_reduced_precision, candidate_block.T, precision=lax.Precision.HIGHEST) - candidate_norm[None, :]) / SOFTMAX_TEMPER
    top = jnp.max(logit_scores, axis=1, keepdims=True)
    log_total = top[:, 0] + jnp.log(jnp.sum(jnp.exp(logit_scores - top), axis=1))
    picked = jnp.take_along_axis(logit_scores, targets[:, None], axis=1)[:, 0]
    losses = log_total - picked
    columns = jnp.arange(logit_scores.shape[1], dtype=jnp.int32)
    onehot = (columns[None, :] == targets[:, None]).astype(jnp.float32)
    softmax_weights = jnp.exp(logit_scores - log_total[:, None]) - onehot
    weights_reduced_precision = lax.optimization_barrier(softmax_weights.astype(jnp.bfloat16)).astype(jnp.float32)
    query_gradient = (2.0 / SOFTMAX_TEMPER) * jnp.dot(weights_reduced_precision, candidate_block, precision=lax.Precision.HIGHEST)
    candidate_gradient = (2.0 / SOFTMAX_TEMPER) * (jnp.dot(weights_reduced_precision.T, query_reduced_precision, precision=lax.Precision.HIGHEST) - jnp.sum(softmax_weights, axis=0)[:, None] * candidate_block)
    real_grad = query_gradient[:, :half_dim]
    imag_grad = query_gradient[:, half_dim:]
    head_grad = jnp.concatenate([real_grad * cosine + imag_grad * sine, imag_grad * cosine - real_grad * sine], axis=1).astype(jnp.bfloat16)
    angle_grad = imag_grad * real_query - real_grad * imag_query
    return losses, head_grad, angle_grad, candidate_gradient


def reference(entity_table, rel_phases, head_ids, rel_ids, target_pos, block_owner, block_local):
    half_dim = rel_phases.shape[1]
    rel_count = rel_phases.shape[0]
    devices = N_ENT * N_GRP
    starts = (block_owner * (ENT_DEV // BLK) + block_local) * BLK
    rows = (starts[:, None] + jnp.arange(BLK, dtype=jnp.int32)[None, :]).reshape(-1).astype(jnp.int32)
    candidate_block = entity_table[rows].astype(jnp.float32)
    candidate_norm = jnp.sum(candidate_block * candidate_block, axis=1)

    def step(carry, inputs):
        cand_total, rel_total = carry
        head_local, rel_local, target_local, device = inputs
        head_rows = ((device // N_GRP) * ENT_DEV + head_local).astype(jnp.int32)
        heads = entity_table[head_rows].astype(jnp.float32)
        angles = rel_phases[rel_local]
        losses, head_grad, angle_grad, candidate_gradient = device_terms(heads, angles, target_local, candidate_block, candidate_norm)
        rel_part = jax.ops.segment_sum(angle_grad, rel_local, num_segments=rel_count)
        return (cand_total + candidate_gradient, rel_total + rel_part), (losses, head_grad)

    start_carry = (jnp.zeros((NBLK * BLK, 2 * half_dim), jnp.float32), jnp.zeros((rel_count, half_dim), jnp.float32))
    inputs = (head_ids.reshape(devices, Q_DEV), rel_ids.reshape(devices, Q_DEV), target_pos.reshape(devices, Q_DEV), jnp.arange(devices, dtype=jnp.int32))
    (cand_total, rel_grad), (losses, head_grad) = lax.scan(step, start_carry, inputs)
    table_grad = jax.ops.segment_sum(cand_total, rows, num_segments=NENT).astype(jnp.bfloat16)
    return losses.reshape(-1), head_grad.reshape(-1, 2 * half_dim), table_grad, rel_grad
```

```python
import functools

import jax
import jax.numpy as jnp
from jax import lax
from jax.experimental import pallas as pl
from jax.experimental.pallas import tpu as pltpu
from jax.sharding import PartitionSpec as P

BLK = 128
SOFTMAX_TEMPER = 2.0
MESH = pl.DeviceIdType.MESH
F32 = jnp.float32
BF16 = jnp.bfloat16
ORDERS = (((1, 2), (2, 2), (4, 4)), ((2, 2), (1, 2), (4, 4)))
SPLIT = 16


class Exchange:
    def __init__(self, acc, stage, recvs, out, send, recv, base, ent, grp, rest):
        self.acc, self.stage, self.recvs, self.out = acc, stage, recvs, out
        self.send, self.recv, self.next = send, recv, base
        self.ent, self.grp, self.rest = ent, grp, rest
        self.length = acc.shape[0]
        self.wide = acc.shape[1] // 2
        self.low = [0, 0]
        self.started = []
        self.live = []

    def go(self, src, dst, ent, grp):
        copy = pltpu.make_async_remote_copy(
            src_ref=src,
            dst_ref=dst,
            send_sem=self.send.at[self.next],
            recv_sem=self.recv.at[self.next],
            device_id=(ent, grp),
            device_id_type=MESH,
        )
        self.next += 1
        copy.start()
        self.started.append(copy)
        self.live.append(copy)

    def land(self):
        for copy in self.live:
            copy.wait_recv()
        self.live = []

    def columns(self, h):
        return pl.ds(h * self.wide, self.wide)

    def rows(self, low, length):
        return pl.ds(pl.multiple_of(low, 16), length)

    def coordinate(self, h, p):
        stride, size = ORDERS[h][p]
        return stride, size, lax.rem(self.ent // stride, size)

    def scatter_start(self, p):
        for h in range(2):
            stride, size, mine = self.coordinate(h, p)
            part = self.length // size
            for k in range(1, size):
                theirs = lax.rem(mine + k, size)
                rows = self.rows(self.low[h] + theirs * part, part)
                self.stage[rows, self.columns(h)] = self.acc[rows, self.columns(h)].astype(BF16)
                self.go(
                    self.stage.at[rows, self.columns(h)],
                    self.recvs[p].at[h, k - 1],
                    self.ent + (theirs - mine) * stride,
                    self.grp,
                )

    def scatter_finish(self, p):
        self.land()
        for h in range(2):
            stride, size, mine = self.coordinate(h, p)
            part = self.length // size
            self.low[h] = self.low[h] + mine * part
            rows = self.rows(self.low[h], part)
            total = self.acc[rows, self.columns(h)]
            for k in range(1, size):
                total = total + self.recvs[p][h, k - 1].astype(F32)
            self.acc[rows, self.columns(h)] = total
        self.length = self.length // ORDERS[0][p][1]

    def across_rest(self):
        if self.rest == 1:
            return
        mine = self.ent // SPLIT
        for h in range(2):
            rows = self.rows(self.low[h], self.length)
            self.stage[rows, self.columns(h)] = self.acc[rows, self.columns(h)].astype(BF16)
            for k in range(1, self.rest):
                theirs = lax.rem(mine + k, self.rest)
                self.go(
                    self.stage.at[rows, self.columns(h)],
                    self.recvs[3].at[h, k - 1],
                    self.ent + (theirs - mine) * SPLIT,
                    self.grp,
                )
        self.land()
        for h in range(2):
            rows = self.rows(self.low[h], self.length)
            total = self.stage[rows, self.columns(h)].astype(F32)
            for k in range(1, self.rest):
                total = total + self.recvs[3][h, k - 1].astype(F32)
            self.acc[rows, self.columns(h)] = total

    def place(self):
        for h in range(2):
            rows = self.rows(self.low[h], self.length)
            self.out[self.grp, rows, self.columns(h)] = self.acc[rows, self.columns(h)].astype(BF16)

    def gather_start(self, p):
        for h in range(2):
            stride, size, mine = self.coordinate(h, p)
            block = self.out.at[self.grp, self.rows(self.low[h], self.length), self.columns(h)]
            for k in range(1, size):
                theirs = lax.rem(mine + k, size)
                self.go(block, block, self.ent + (theirs - mine) * stride, self.grp)

    def gather_finish(self, p):
        self.land()
        for h in range(2):
            _, _, mine = self.coordinate(h, p)
            self.low[h] = self.low[h] - mine * self.length
        self.length = self.length * ORDERS[0][p][1]

    def sibling(self):
        self.go(self.out.at[self.grp], self.out.at[self.grp], self.ent, 1 - self.grp)
        self.land()

    def finish(self):
        for copy in self.started:
            copy.wait_send()


def kernel(
    n_ent,
    block_owner,
    block_local,
    table,
    phases,
    head_ids,
    rel_ids,
    target_pos,
    losses_out,
    head_out,
    table_out,
    rel_out,
    c_acc,
    c_stage,
    cands,
    g_acc,
    g_stage,
    grads,
    s_stage,
    s_recv,
    c_r0,
    c_r1,
    c_r2,
    c_r3,
    g_r0,
    g_r1,
    g_r2,
    g_r3,
    padded,
    queries,
    send,
    recv,
):
    ent = lax.axis_index("ent")
    grp = lax.axis_index("grp")
    rest = n_ent // SPLIT
    half = phases.shape[1]
    rel_count = phases.shape[0]
    rel_half = padded.shape[0] // 2
    n_cand = c_acc.shape[0]
    blocks = n_cand // BLK
    q_dev = head_ids.shape[1]

    barrier = pltpu.get_barrier_semaphore()
    partners = [(ent, 1 - grp)]
    for stride, size in ORDERS[0] + ((SPLIT, rest),):
        mine = lax.rem(ent // stride, size)
        for k in range(1, size):
            partners.append((ent + (lax.rem(mine + k, size) - mine) * stride, grp))
    for partner in partners:
        pl.semaphore_signal(barrier, inc=1, device_id=partner, device_id_type=MESH)

    my_columns = pl.ds(pl.multiple_of(grp * half, 128), half)
    for b in range(blocks):
        total = jnp.zeros((BLK, half), F32)
        for local in range(table.shape[0] // BLK):
            wanted = jnp.logical_and(block_owner[b] == ent, block_local[b] == local)
            value = table[pl.ds(local * BLK, BLK), my_columns].astype(F32)
            total = jnp.where(wanted, value, total)
        c_acc[pl.ds(b * BLK, BLK), :] = total

    pl.semaphore_wait(barrier, len(partners))

    fetch = Exchange(c_acc, c_stage, (c_r0, c_r1, c_r2, c_r3), cands, send, recv, 0, ent, grp, rest)
    fetch.scatter_start(0)

    rows_t = lax.broadcasted_iota(jnp.int32, (table.shape[0], q_dev), 0)
    head_pick = (rows_t == head_ids[...]).astype(F32).T.astype(BF16)
    heads = jnp.dot(head_pick, table[...], preferred_element_type=F32)
    padded[...] = jnp.zeros_like(padded)
    padded[pl.ds(0, rel_count), :] = phases[...]
    rel_rows = lax.broadcasted_iota(jnp.int32, (2 * rel_half, q_dev), 0)
    rel_pick = (rel_rows == rel_ids[...]).astype(F32).T.astype(BF16)

    fetch.scatter_finish(0)
    fetch.scatter_start(1)

    whole = padded[...]
    top_part = whole.astype(BF16)
    left = whole - top_part.astype(F32)
    mid_part = left.astype(BF16)
    low_part = (left - mid_part.astype(F32)).astype(BF16)
    angles = (
        jnp.dot(rel_pick, low_part, preferred_element_type=F32)
        + jnp.dot(rel_pick, mid_part, preferred_element_type=F32)
    ) + jnp.dot(rel_pick, top_part, preferred_element_type=F32)

    fetch.scatter_finish(1)
    fetch.scatter_start(2)

    cosine = jnp.cos(angles)
    sine = jnp.sin(angles)

    fetch.scatter_finish(2)
    fetch.across_rest()
    fetch.place()
    fetch.gather_start(2)

    real_head = heads[:, :half]
    imag_head = heads[:, half:]
    real_query = real_head * cosine - imag_head * sine
    imag_query = real_head * sine + imag_head * cosine
    queries[0] = real_query.astype(BF16)
    queries[1] = imag_query.astype(BF16)

    fetch.gather_finish(2)
    fetch.gather_start(1)
    fetch.gather_finish(1)
    fetch.gather_start(0)
    fetch.gather_finish(0)
    fetch.sibling()

    contract_last = (((1,), (1,)), ((), ()))
    cand_real = cands[0]
    cand_imag = cands[1]
    inner = lax.dot_general(cand_real, queries[0], contract_last, preferred_element_type=F32)
    inner = inner + lax.dot_general(cand_imag, queries[1], contract_last, preferred_element_type=F32)
    norm = jnp.sum(jnp.square(cand_real.astype(F32)), axis=1, keepdims=True)
    norm = norm + jnp.sum(jnp.square(cand_imag.astype(F32)), axis=1, keepdims=True)
    scores = (2.0 * inner - norm) / SOFTMAX_TEMPER
    top = jnp.max(scores, axis=0, keepdims=True)
    log_total = top + jnp.log(jnp.sum(jnp.exp(scores - top), axis=0, keepdims=True))
    target = lax.broadcasted_iota(jnp.int32, (n_cand, q_dev), 0) == target_pos[...]
    losses_out[...] = log_total - jnp.sum(jnp.where(target, scores, 0.0), axis=0, keepdims=True)
    weights = jnp.exp(scores - log_total) - target.astype(F32)
    weights_low = weights.astype(BF16)
    weight_sums = jnp.sum(weights, axis=1, keepdims=True)
    weights_by_query = weights.T.astype(BF16)
    scale = 2.0 / SOFTMAX_TEMPER
    real_grad = scale * jnp.dot(weights_by_query, cand_real, preferred_element_type=F32)
    imag_grad = scale * jnp.dot(weights_by_query, cand_imag, preferred_element_type=F32)
    angle_grad = imag_grad * real_query - real_grad * imag_query
    angle_high = angle_grad.astype(BF16)
    angle_low = (angle_grad - angle_high.astype(F32)).astype(BF16)

    def part_of(side):
        cand_part = scale * (
            jnp.dot(weights_low, queries[side], preferred_element_type=F32)
            - weight_sums * cands[side].astype(F32)
        )
        rows = lax.broadcasted_iota(jnp.int32, (rel_half, q_dev), 0) + side * rel_half
        pick = (rows == rel_ids[...]).astype(F32).astype(BF16)
        rel_part = jnp.dot(pick, angle_high, preferred_element_type=F32)
        rel_part = rel_part + jnp.dot(pick, angle_low, preferred_element_type=F32)
        return cand_part, rel_part

    reduce = Exchange(
        g_acc, g_stage, (g_r0, g_r1, g_r2, g_r3), grads, send, recv, fetch.next, ent, grp, rest
    )
    cand_part, rel_part = part_of(1 - grp)
    s_stage[pl.ds(0, n_cand), :] = cand_part.astype(BF16)
    s_stage[pl.ds(n_cand, rel_half), :] = rel_part.astype(BF16)
    reduce.go(s_stage, s_recv, ent, 1 - grp)
    cand_part, rel_part = part_of(grp)
    g_acc[pl.ds(0, n_cand), :] = cand_part
    g_acc[pl.ds(n_cand, rel_half), :] = rel_part
    reduce.land()
    g_acc[...] += s_recv[...].astype(F32)
    reduce.scatter_start(0)

    head_out[:, pl.ds(0, half)] = (real_grad * cosine + imag_grad * sine).astype(BF16)
    head_out[:, pl.ds(half, half)] = (imag_grad * cosine - real_grad * sine).astype(BF16)

    reduce.scatter_finish(0)
    reduce.scatter_start(1)
    reduce.scatter_finish(1)
    reduce.scatter_start(2)
    reduce.scatter_finish(2)
    reduce.across_rest()
    reduce.place()
    for p in (2, 1, 0):
        reduce.gather_start(p)
        reduce.gather_finish(p)
    reduce.sibling()

    for local in range(table.shape[0] // BLK):
        for side in range(2):
            total = jnp.zeros((BLK, half), F32)
            for b in range(blocks):
                mine = jnp.logical_and(block_owner[b] == ent, block_local[b] == local)
                value = grads[side, pl.ds(b * BLK, BLK), :].astype(F32)
                total = total + jnp.where(mine, value, 0.0)
            table_out[pl.ds(local * BLK, BLK), pl.ds(side * half, half)] = total.astype(BF16)
    rel_out[pl.ds(0, rel_half), :] = grads[0, pl.ds(n_cand, rel_half), :].astype(F32)
    tail = rel_count - rel_half
    rel_out[pl.ds(rel_half, tail), :] = grads[1, pl.ds(n_cand, rel_half), :].astype(F32)[:tail]
    fetch.finish()
    reduce.finish()


def body(n_ent, entity_table, rel_phases, head_ids, rel_ids, target_pos, block_owner, block_local):
    rel_count, half = rel_phases.shape
    shard_rows = entity_table.shape[0]
    q_dev = head_ids.shape[0]
    n_cand = block_owner.shape[0] * BLK
    rel_half = -(-rel_count // (2 * 256)) * 256
    g_rows = n_cand + rel_half
    rest = n_ent // SPLIT
    copies = 2 * (2 * 2 * (1 + 1 + 3) + 2 * (rest - 1) + 1) + 1

    def slots(rows):
        quarter = half // 2
        return [
            pltpu.VMEM((2, 1, rows // 2, quarter), BF16),
            pltpu.VMEM((2, 1, rows // 4, quarter), BF16),
            pltpu.VMEM((2, 3, rows // 16, quarter), BF16),
            pltpu.VMEM((2, max(rest - 1, 1), rows // 16, quarter), BF16),
        ]

    vmem = pl.BlockSpec(memory_space=pltpu.VMEM)
    smem = pl.BlockSpec(memory_space=pltpu.SMEM)
    losses, head_grad, table_grad, rel_grad = pl.pallas_call(
        functools.partial(kernel, n_ent),
        out_shape=(
            jax.ShapeDtypeStruct((1, q_dev), F32),
            jax.ShapeDtypeStruct((q_dev, 2 * half), BF16),
            jax.ShapeDtypeStruct((shard_rows, 2 * half), BF16),
            jax.ShapeDtypeStruct((rel_count, half), F32),
        ),
        in_specs=[smem, smem] + [vmem] * 5,
        out_specs=(vmem,) * 4,
        scratch_shapes=[
            pltpu.VMEM((n_cand, half), F32),
            pltpu.VMEM((n_cand, half), BF16),
            pltpu.VMEM((2, n_cand, half), BF16),
            pltpu.VMEM((g_rows, half), F32),
            pltpu.VMEM((g_rows, half), BF16),
            pltpu.VMEM((2, g_rows, half), BF16),
            pltpu.VMEM((g_rows, half), BF16),
            pltpu.VMEM((g_rows, half), BF16),
            *slots(n_cand),
            *slots(g_rows),
            pltpu.VMEM((2 * rel_half, half), F32),
            pltpu.VMEM((2, q_dev, half), BF16),
            pltpu.SemaphoreType.DMA((copies,)),
            pltpu.SemaphoreType.DMA((copies,)),
        ],
        compiler_params=pltpu.CompilerParams(collective_id=0, has_side_effects=True),
    )(
        block_owner,
        block_local,
        entity_table,
        rel_phases,
        head_ids.reshape(1, q_dev),
        rel_ids.reshape(1, q_dev),
        target_pos.reshape(1, q_dev),
    )
    return losses.reshape(q_dev), head_grad, table_grad, rel_grad


def solution(mesh):
    return jax.shard_map(
        functools.partial(body, mesh.shape["ent"]),
        mesh=mesh,
        in_specs=(
            P("ent", None),
            P(),
            P(("ent", "grp")),
            P(("ent", "grp")),
            P(("ent", "grp")),
            P(),
            P(),
        ),
        out_specs=(P(("ent", "grp")), P(("ent", "grp"), None), P("ent", None), P()),
        check_vma=False,
    )
```

```python
import functools

import jax
import jax.numpy as jnp
from jax import lax
from jax.experimental import pallas as pl
from jax.experimental.pallas import tpu as pltpu
from jax.sharding import PartitionSpec as P

BLK = 128
SOFTMAX_TEMPER = 2.0
MESH = pl.DeviceIdType.MESH
F32 = jnp.float32
BF16 = jnp.bfloat16
ORDERS = (((1, 2), (2, 2)), ((2, 2), (1, 2)))
LINE = (4, 4)
SPLIT = 16
CHUNK = 128


class Exchange:
    def __init__(self, refs, low, length, order, sems, place):
        self.acc, self.stage, self.out, self.slots = refs
        self.base, self.low, self.length, self.order = low, low, length, ORDERS[order]
        self.sems = sems
        self.ent, self.grp, self.rest = place
        self.wide = self.acc.shape[1] // LINE[1]
        self.started = []
        self.live = []
        self.step = 0

    def go(self, src, dst, ent, grp):
        send, recv = self.sems
        number = len(send[1])
        send[1].append(number)
        copy = pltpu.make_async_remote_copy(
            src_ref=src,
            dst_ref=dst,
            send_sem=send[0].at[number],
            recv_sem=recv.at[number],
            device_id=(ent, grp),
            device_id_type=MESH,
        )
        copy.start()
        self.started.append(copy)
        self.live.append(copy)

    def land(self):
        for copy in self.live:
            copy.wait_recv()
        self.live = []

    def rows(self, low, length):
        return pl.ds(pl.multiple_of(low, 16), length)

    def tile(self, number):
        return pl.ds(pl.multiple_of(number * self.wide, 128), self.wide)

    def coordinate(self, stride, size):
        return lax.rem(self.ent // stride, size)

    def peers(self, stride, size):
        mine = self.coordinate(stride, size)
        for k in range(1, size):
            theirs = lax.rem(mine + k, size)
            yield k - 1, theirs, self.ent + (theirs - mine) * stride

    def scatter_start(self, p):
        stride, size = self.order[p]
        part = self.length // size
        for _, theirs, peer in self.peers(stride, size):
            rows = self.rows(self.low + theirs * part, part)
            self.stage[rows, :] = self.acc[rows, :].astype(BF16)
            slot = self.slots[p].at[pl.ds(self.base // (2 << p), part), :]
            self.go(self.stage.at[rows, :], slot, peer, self.grp)

    def scatter_finish(self, p):
        self.land()
        stride, size = self.order[p]
        part = self.length // size
        self.low = self.low + self.coordinate(stride, size) * part
        self.length = part
        rows = self.rows(self.low, part)
        self.acc[rows, :] += self.slots[p][pl.ds(self.base // (2 << p), part), :].astype(F32)

    def line_start(self):
        rows = self.rows(self.low, self.length)
        self.stage[rows, :] = self.acc[rows, :].astype(BF16)
        for k, theirs, peer in self.peers(*LINE):
            slot = self.slots[2].at[k, pl.ds(self.base // 4, self.length), :]
            self.go(self.stage.at[rows, self.tile(theirs)], slot, peer, self.grp)

    def line_finish(self):
        self.land()
        rows = self.rows(self.low, self.length)
        mine = self.tile(self.coordinate(*LINE))
        total = self.acc[rows, mine]
        for k in range(LINE[1] - 1):
            total = total + self.slots[2][k, pl.ds(self.base // 4, self.length), :].astype(F32)
        if self.rest > 1:
            self.stage[rows, mine] = total.astype(BF16)
            for k, _, peer in self.peers(SPLIT, self.rest):
                slot = self.slots[3].at[k, pl.ds(self.base // 4, self.length), :]
                self.go(self.stage.at[rows, mine], slot, peer, self.grp)
            self.land()
            total = self.stage[rows, mine].astype(F32)
            for k in range(self.rest - 1):
                total = total + self.slots[3][k, pl.ds(self.base // 4, self.length), :].astype(F32)
        self.out[self.grp, rows, mine] = total.astype(BF16)

    def line_gather_start(self):
        rows = self.rows(self.low, self.length)
        block = self.out.at[self.grp, rows, self.tile(self.coordinate(*LINE))]
        for _, _, peer in self.peers(*LINE):
            self.go(block, block, peer, self.grp)

    def gather_start(self, p):
        block = self.out.at[self.grp, self.rows(self.low, self.length), :]
        for _, _, peer in self.peers(*self.order[p]):
            self.go(block, block, peer, self.grp)

    def gather_finish(self, p):
        self.land()
        self.low = self.low - self.coordinate(*self.order[p]) * self.length
        self.length = self.length * self.order[p][1]

    def sibling_start(self):
        block = self.out.at[self.grp, pl.ds(self.base, self.length), :]
        self.go(block, block, self.ent, 1 - self.grp)

    def advance(self):
        if self.step == 0:
            self.scatter_start(0)
        elif self.step == 1:
            self.scatter_finish(0)
            self.scatter_start(1)
        elif self.step == 2:
            self.scatter_finish(1)
            self.line_start()
        elif self.step == 3:
            self.line_finish()
            self.line_gather_start()
        elif self.step == 4:
            self.land()
            self.gather_start(1)
        elif self.step == 5:
            self.gather_finish(1)
            self.gather_start(0)
        elif self.step == 6:
            self.gather_finish(0)
            self.sibling_start()
        elif self.step == 7:
            self.land()
        self.step += 1

    def finish(self):
        for copy in self.started:
            copy.wait_send()


def chunks(total, length):
    return [(low, min(length, total - low)) for low in range(0, total, length)]


def kernel(
    n_ent,
    block_owner,
    block_local,
    table,
    phases,
    head_ids,
    rel_ids,
    target_pos,
    losses_out,
    head_out,
    table_out,
    rel_out,
    c_acc,
    c_stage,
    cands,
    g_acc,
    g_stage,
    grads,
    s_stage,
    s_recv,
    c_r0,
    c_r1,
    c_r2,
    c_r3,
    g_r0,
    g_r1,
    g_r2,
    g_r3,
    padded,
    queries,
    send,
    recv,
):
    ent = lax.axis_index("ent")
    grp = lax.axis_index("grp")
    rest = n_ent // SPLIT
    half = phases.shape[1]
    rel_count = phases.shape[0]
    rel_half = padded.shape[0] // 2
    n_cand = c_acc.shape[0]
    blocks = n_cand // BLK
    q_dev = head_ids.shape[1]

    barrier = pltpu.get_barrier_semaphore()
    partners = [(ent, 1 - grp)]
    for stride, size in ORDERS[0] + (LINE, (SPLIT, rest)):
        mine = lax.rem(ent // stride, size)
        for k in range(1, size):
            partners.append((ent + (lax.rem(mine + k, size) - mine) * stride, grp))
    for partner in partners:
        pl.semaphore_signal(barrier, inc=1, device_id=partner, device_id_type=MESH)

    my_columns = pl.ds(pl.multiple_of(grp * half, 128), half)
    for b in range(blocks):
        total = jnp.zeros((BLK, half), F32)
        for local in range(table.shape[0] // BLK):
            wanted = jnp.logical_and(block_owner[b] == ent, block_local[b] == local)
            value = table[pl.ds(local * BLK, BLK), my_columns].astype(F32)
            total = jnp.where(wanted, value, total)
        c_acc[pl.ds(b * BLK, BLK), :] = total

    pl.semaphore_wait(barrier, len(partners))

    place = (ent, grp, rest)
    sems = ((send, []), recv)
    refs = (c_acc, c_stage, cands, (c_r0, c_r1, c_r2, c_r3))
    fetch = [
        Exchange(refs, low, length, i % 2, sems, place)
        for i, (low, length) in enumerate(chunks(n_cand, CHUNK))
    ]

    def advance(group):
        for exchange in group:
            exchange.advance()

    advance(fetch)

    rows_t = lax.broadcasted_iota(jnp.int32, (table.shape[0], q_dev), 0)
    head_pick = (rows_t == head_ids[...]).astype(F32).T.astype(BF16)
    heads = jnp.dot(head_pick, table[...], preferred_element_type=F32)
    padded[...] = jnp.zeros_like(padded)
    padded[pl.ds(0, rel_count), :] = phases[...]
    rel_rows = lax.broadcasted_iota(jnp.int32, (2 * rel_half, q_dev), 0)
    rel_pick = (rel_rows == rel_ids[...]).astype(F32).T.astype(BF16)

    advance(fetch)

    whole = padded[...]
    top_part = whole.astype(BF16)
    left = whole - top_part.astype(F32)
    mid_part = left.astype(BF16)
    low_part = (left - mid_part.astype(F32)).astype(BF16)
    angles = (
        jnp.dot(rel_pick, low_part, preferred_element_type=F32)
        + jnp.dot(rel_pick, mid_part, preferred_element_type=F32)
    ) + jnp.dot(rel_pick, top_part, preferred_element_type=F32)

    advance(fetch)

    cosine = jnp.cos(angles)
    sine = jnp.sin(angles)

    advance(fetch)

    real_head = heads[:, :half]
    imag_head = heads[:, half:]
    real_query = real_head * cosine - imag_head * sine
    imag_query = real_head * sine + imag_head * cosine
    queries[0] = real_query.astype(BF16)
    queries[1] = imag_query.astype(BF16)

    for _ in range(4):
        advance(fetch)

    contract_last = (((1,), (1,)), ((), ()))
    cand_real = cands[0]
    cand_imag = cands[1]
    inner = lax.dot_general(cand_real, queries[0], contract_last, preferred_element_type=F32)
    inner = inner + lax.dot_general(cand_imag, queries[1], contract_last, preferred_element_type=F32)
    norm = jnp.sum(jnp.square(cand_real.astype(F32)), axis=1, keepdims=True)
    norm = norm + jnp.sum(jnp.square(cand_imag.astype(F32)), axis=1, keepdims=True)
    scores = (2.0 * inner - norm) / SOFTMAX_TEMPER
    top = jnp.max(scores, axis=0, keepdims=True)
    log_total = top + jnp.log(jnp.sum(jnp.exp(scores - top), axis=0, keepdims=True))
    target = lax.broadcasted_iota(jnp.int32, (n_cand, q_dev), 0) == target_pos[...]
    losses_out[...] = log_total - jnp.sum(jnp.where(target, scores, 0.0), axis=0, keepdims=True)
    weights = jnp.exp(scores - log_total) - target.astype(F32)
    weights_low = weights.astype(BF16)
    weight_sums = jnp.sum(weights, axis=1, keepdims=True)
    weights_by_query = weights.T.astype(BF16)
    scale = 2.0 / SOFTMAX_TEMPER

    def cand_part(side):
        return scale * (
            jnp.dot(weights_low, queries[side], preferred_element_type=F32)
            - weight_sums * cands[side].astype(F32)
        )

    refs = (g_acc, g_stage, grads, (g_r0, g_r1, g_r2, g_r3))
    cand_reduce = [
        Exchange(refs, low, length, i % 2, sems, place)
        for i, (low, length) in enumerate(chunks(n_cand, CHUNK))
    ]
    rel_reduce = [
        Exchange(refs, n_cand + low, length, i % 2, sems, place)
        for i, (low, length) in enumerate(chunks(rel_half, CHUNK))
    ]

    def swap(group):
        for exchange in group:
            rows = pl.ds(exchange.base, exchange.length)
            exchange.go(s_stage.at[rows, :], s_recv.at[rows, :], ent, 1 - grp)

    def merge(group):
        for exchange in group:
            exchange.land()
            rows = pl.ds(exchange.base, exchange.length)
            g_acc[rows, :] += s_recv[rows, :].astype(F32)
            exchange.advance()

    s_stage[pl.ds(0, n_cand), :] = cand_part(1 - grp).astype(BF16)
    swap(cand_reduce)
    g_acc[pl.ds(0, n_cand), :] = cand_part(grp)
    merge(cand_reduce)

    real_grad = scale * jnp.dot(weights_by_query, cand_real, preferred_element_type=F32)
    imag_grad = scale * jnp.dot(weights_by_query, cand_imag, preferred_element_type=F32)
    angle_grad = imag_grad * real_query - real_grad * imag_query
    angle_high = angle_grad.astype(BF16)
    angle_low = (angle_grad - angle_high.astype(F32)).astype(BF16)

    def rel_part(side):
        rows = lax.broadcasted_iota(jnp.int32, (rel_half, q_dev), 0) + side * rel_half
        pick = (rows == rel_ids[...]).astype(F32).astype(BF16)
        return jnp.dot(pick, angle_high, preferred_element_type=F32) + jnp.dot(
            pick, angle_low, preferred_element_type=F32
        )

    s_stage[pl.ds(n_cand, rel_half), :] = rel_part(1 - grp).astype(BF16)
    swap(rel_reduce)
    g_acc[pl.ds(n_cand, rel_half), :] = rel_part(grp)
    advance(cand_reduce)
    merge(rel_reduce)

    head_out[:, pl.ds(0, half)] = (real_grad * cosine + imag_grad * sine).astype(BF16)
    head_out[:, pl.ds(half, half)] = (imag_grad * cosine - real_grad * sine).astype(BF16)

    for _ in range(6):
        advance(cand_reduce)
        advance(rel_reduce)

    for local in range(table.shape[0] // BLK):
        for side in range(2):
            total = jnp.zeros((BLK, half), F32)
            for b in range(blocks):
                mine = jnp.logical_and(block_owner[b] == ent, block_local[b] == local)
                value = grads[side, pl.ds(b * BLK, BLK), :].astype(F32)
                total = total + jnp.where(mine, value, 0.0)
            table_out[pl.ds(local * BLK, BLK), pl.ds(side * half, half)] = total.astype(BF16)
    advance(rel_reduce)
    rel_out[pl.ds(0, rel_half), :] = grads[0, pl.ds(n_cand, rel_half), :].astype(F32)
    tail = rel_count - rel_half
    rel_out[pl.ds(rel_half, tail), :] = grads[1, pl.ds(n_cand, rel_half), :].astype(F32)[:tail]
    for exchange in fetch + cand_reduce + rel_reduce:
        exchange.finish()


def body(n_ent, entity_table, rel_phases, head_ids, rel_ids, target_pos, block_owner, block_local):
    rel_count, half = rel_phases.shape
    shard_rows = entity_table.shape[0]
    q_dev = head_ids.shape[0]
    n_cand = block_owner.shape[0] * BLK
    rel_half = -(-rel_count // (2 * 64)) * 64
    g_rows = n_cand + rel_half
    rest = n_ent // SPLIT
    cand_chunks, rel_chunks = len(chunks(n_cand, CHUNK)), len(chunks(rel_half, CHUNK))
    each = 2 * (1 + 1 + 3) + 1 + rest - 1
    copies = each * (2 * cand_chunks + rel_chunks) + cand_chunks + rel_chunks

    def slots(rows):
        tile = half // LINE[1]
        return [
            pltpu.VMEM((rows // 2, half), BF16),
            pltpu.VMEM((rows // 4, half), BF16),
            pltpu.VMEM((3, rows // 4, tile), BF16),
            pltpu.VMEM((max(rest - 1, 1), rows // 4, tile), BF16),
        ]

    vmem = pl.BlockSpec(memory_space=pltpu.VMEM)
    smem = pl.BlockSpec(memory_space=pltpu.SMEM)
    losses, head_grad, table_grad, rel_grad = pl.pallas_call(
        functools.partial(kernel, n_ent),
        out_shape=(
            jax.ShapeDtypeStruct((1, q_dev), F32),
            jax.ShapeDtypeStruct((q_dev, 2 * half), BF16),
            jax.ShapeDtypeStruct((shard_rows, 2 * half), BF16),
            jax.ShapeDtypeStruct((rel_count, half), F32),
        ),
        in_specs=[smem, smem] + [vmem] * 5,
        out_specs=(vmem,) * 4,
        scratch_shapes=[
            pltpu.VMEM((n_cand, half), F32),
            pltpu.VMEM((n_cand, half), BF16),
            pltpu.VMEM((2, n_cand, half), BF16),
            pltpu.VMEM((g_rows, half), F32),
            pltpu.VMEM((g_rows, half), BF16),
            pltpu.VMEM((2, g_rows, half), BF16),
            pltpu.VMEM((g_rows, half), BF16),
            pltpu.VMEM((g_rows, half), BF16),
            *slots(n_cand),
            *slots(g_rows),
            pltpu.VMEM((2 * rel_half, half), F32),
            pltpu.VMEM((2, q_dev, half), BF16),
            pltpu.SemaphoreType.DMA((copies,)),
            pltpu.SemaphoreType.DMA((copies,)),
        ],
        compiler_params=pltpu.CompilerParams(collective_id=0, has_side_effects=True),
    )(
        block_owner,
        block_local,
        entity_table,
        rel_phases,
        head_ids.reshape(1, q_dev),
        rel_ids.reshape(1, q_dev),
        target_pos.reshape(1, q_dev),
    )
    return losses.reshape(q_dev), head_grad, table_grad, rel_grad


def solution(mesh):
    return jax.shard_map(
        functools.partial(body, mesh.shape["ent"]),
        mesh=mesh,
        in_specs=(
            P("ent", None),
            P(),
            P(("ent", "grp")),
            P(("ent", "grp")),
            P(("ent", "grp")),
            P(),
            P(),
        ),
        out_specs=(P(("ent", "grp")), P(("ent", "grp"), None), P("ent", None), P()),
        check_vma=False,
    )
```

```python
import functools

import jax
import jax.numpy as jnp
from jax import lax
from jax.experimental import pallas as pl
from jax.experimental.pallas import tpu as pltpu
from jax.sharding import PartitionSpec as P

BLK = 128
SOFTMAX_TEMPER = 2.0
MESH = pl.DeviceIdType.MESH
F32 = jnp.float32
BF16 = jnp.bfloat16
ORDERS = (((1, 2), (2, 2)), ((2, 2), (1, 2)))
LINE = (4, 4)
SPLIT = 16
CHUNK = 128


class Exchange:
    def __init__(self, refs, low, length, order, sems, place):
        self.acc, self.stage, self.out, self.slots = refs
        self.base, self.low, self.length, self.order = low, low, length, ORDERS[order]
        self.sems = sems
        self.ent, self.grp, self.rest = place
        self.wide = self.acc.shape[1] // LINE[1]
        self.started = []
        self.live = []
        self.step = 0

    def go(self, src, dst, ent, grp):
        send, recv = self.sems
        number = len(send[1])
        send[1].append(number)
        copy = pltpu.make_async_remote_copy(
            src_ref=src,
            dst_ref=dst,
            send_sem=send[0].at[number],
            recv_sem=recv.at[number],
            device_id=(ent, grp),
            device_id_type=MESH,
        )
        copy.start()
        self.started.append(copy)
        self.live.append(copy)

    def land(self):
        for copy in self.live:
            copy.wait_recv()
        self.live = []

    def rows(self, low, length):
        return pl.ds(pl.multiple_of(low, 16), length)

    def tile(self, number):
        return pl.ds(pl.multiple_of(number * self.wide, 128), self.wide)

    def coordinate(self, stride, size):
        return lax.rem(self.ent // stride, size)

    def peers(self, stride, size):
        mine = self.coordinate(stride, size)
        for k in range(1, size):
            theirs = lax.rem(mine + k, size)
            yield k - 1, theirs, self.ent + (theirs - mine) * stride

    def scatter_start(self, p):
        stride, size = self.order[p]
        part = self.length // size
        for _, theirs, peer in self.peers(stride, size):
            rows = self.rows(self.low + theirs * part, part)
            self.stage[rows, :] = self.acc[rows, :].astype(BF16)
            slot = self.slots[p].at[pl.ds(self.base // (2 << p), part), :]
            self.go(self.stage.at[rows, :], slot, peer, self.grp)

    def scatter_finish(self, p):
        self.land()
        stride, size = self.order[p]
        part = self.length // size
        self.low = self.low + self.coordinate(stride, size) * part
        self.length = part
        rows = self.rows(self.low, part)
        self.acc[rows, :] += self.slots[p][pl.ds(self.base // (2 << p), part), :].astype(F32)

    def line_start(self):
        rows = self.rows(self.low, self.length)
        self.stage[rows, :] = self.acc[rows, :].astype(BF16)
        for k, theirs, peer in self.peers(*LINE):
            slot = self.slots[2].at[k, pl.ds(self.base // 4, self.length), :]
            self.go(self.stage.at[rows, self.tile(theirs)], slot, peer, self.grp)

    def line_finish(self):
        self.land()
        rows = self.rows(self.low, self.length)
        mine = self.tile(self.coordinate(*LINE))
        total = self.acc[rows, mine]
        for k in range(LINE[1] - 1):
            total = total + self.slots[2][k, pl.ds(self.base // 4, self.length), :].astype(F32)
        if self.rest > 1:
            self.stage[rows, mine] = total.astype(BF16)
            for k, _, peer in self.peers(SPLIT, self.rest):
                slot = self.slots[3].at[k, pl.ds(self.base // 4, self.length), :]
                self.go(self.stage.at[rows, mine], slot, peer, self.grp)
            self.land()
            total = self.stage[rows, mine].astype(F32)
            for k in range(self.rest - 1):
                total = total + self.slots[3][k, pl.ds(self.base // 4, self.length), :].astype(F32)
        self.out[self.grp, rows, mine] = total.astype(BF16)

    def line_gather_start(self):
        rows = self.rows(self.low, self.length)
        block = self.out.at[self.grp, rows, self.tile(self.coordinate(*LINE))]
        for _, _, peer in self.peers(*LINE):
            self.go(block, block, peer, self.grp)

    def gather_start(self, p):
        block = self.out.at[self.grp, self.rows(self.low, self.length), :]
        for _, _, peer in self.peers(*self.order[p]):
            self.go(block, block, peer, self.grp)

    def gather_finish(self, p):
        self.land()
        self.low = self.low - self.coordinate(*self.order[p]) * self.length
        self.length = self.length * self.order[p][1]

    def sibling_start(self):
        block = self.out.at[self.grp, pl.ds(self.base, self.length), :]
        self.go(block, block, self.ent, 1 - self.grp)

    def advance(self):
        if self.step == 0:
            self.scatter_start(0)
        elif self.step == 1:
            self.scatter_finish(0)
            self.scatter_start(1)
        elif self.step == 2:
            self.scatter_finish(1)
            self.line_start()
        elif self.step == 3:
            self.line_finish()
            self.line_gather_start()
        elif self.step == 4:
            self.land()
            self.gather_start(1)
        elif self.step == 5:
            self.gather_finish(1)
            self.gather_start(0)
        elif self.step == 6:
            self.gather_finish(0)
            self.sibling_start()
        elif self.step == 7:
            self.land()
        self.step += 1

    def finish(self):
        for copy in self.started:
            copy.wait_send()


def chunks(total, length):
    return [(low, min(length, total - low)) for low in range(0, total, length)]


def kernel(
    n_ent,
    block_owner,
    block_local,
    table,
    phases,
    head_ids,
    rel_ids,
    target_pos,
    losses_out,
    head_any,
    grads_any,
    c_acc,
    c_stage,
    cands,
    g_acc,
    g_stage,
    grads,
    s_stage,
    s_recv,
    c_r0,
    c_r1,
    c_r2,
    c_r3,
    g_r0,
    g_r1,
    g_r2,
    g_r3,
    loaded,
    padded,
    queries,
    head_out,
    local_sem,
    send,
    recv,
):
    ent = lax.axis_index("ent")
    grp = lax.axis_index("grp")
    rest = n_ent // SPLIT
    half = phases.shape[1]
    rel_count = phases.shape[0]
    rel_half = padded.shape[0] // 2
    n_cand = c_acc.shape[0]
    blocks = n_cand // BLK
    q_dev = head_ids.shape[1]

    load = pltpu.make_async_copy(phases, loaded, local_sem.at[0])
    load.start()
    barrier = pltpu.get_barrier_semaphore()
    partners = [(ent, 1 - grp)]
    for stride, size in ORDERS[0] + (LINE, (SPLIT, rest)):
        mine = lax.rem(ent // stride, size)
        for k in range(1, size):
            partners.append((ent + (lax.rem(mine + k, size) - mine) * stride, grp))
    for partner in partners:
        pl.semaphore_signal(barrier, inc=1, device_id=partner, device_id_type=MESH)

    my_columns = pl.ds(pl.multiple_of(grp * half, 128), half)
    for b in range(blocks):
        total = jnp.zeros((BLK, half), F32)
        for local in range(table.shape[0] // BLK):
            wanted = jnp.logical_and(block_owner[b] == ent, block_local[b] == local)
            value = table[pl.ds(local * BLK, BLK), my_columns].astype(F32)
            total = jnp.where(wanted, value, total)
        c_acc[pl.ds(b * BLK, BLK), :] = total

    pl.semaphore_wait(barrier, len(partners))

    place = (ent, grp, rest)
    sems = ((send, []), recv)
    refs = (c_acc, c_stage, cands, (c_r0, c_r1, c_r2, c_r3))
    fetch = [
        Exchange(refs, low, length, i % 2, sems, place)
        for i, (low, length) in enumerate(chunks(n_cand, CHUNK))
    ]

    def advance(group):
        for exchange in group:
            exchange.advance()

    advance(fetch)

    rows_t = lax.broadcasted_iota(jnp.int32, (table.shape[0], q_dev), 0)
    head_pick = (rows_t == head_ids[...]).astype(F32).T.astype(BF16)
    heads = jnp.dot(head_pick, table[...], preferred_element_type=F32)
    rel_rows = lax.broadcasted_iota(jnp.int32, (2 * rel_half, q_dev), 0)
    rel_pick = (rel_rows == rel_ids[...]).astype(F32).T.astype(BF16)

    advance(fetch)

    load.wait()
    padded[...] = jnp.zeros_like(padded)
    padded[pl.ds(0, rel_count), :] = loaded[...]
    whole = padded[...]
    top_part = whole.astype(BF16)
    left = whole - top_part.astype(F32)
    mid_part = left.astype(BF16)
    low_part = (left - mid_part.astype(F32)).astype(BF16)
    angles = (
        jnp.dot(rel_pick, low_part, preferred_element_type=F32)
        + jnp.dot(rel_pick, mid_part, preferred_element_type=F32)
    ) + jnp.dot(rel_pick, top_part, preferred_element_type=F32)

    advance(fetch)

    cosine = jnp.cos(angles)
    sine = jnp.sin(angles)

    advance(fetch)

    real_head = heads[:, :half]
    imag_head = heads[:, half:]
    real_query = real_head * cosine - imag_head * sine
    imag_query = real_head * sine + imag_head * cosine
    queries[0] = real_query.astype(BF16)
    queries[1] = imag_query.astype(BF16)

    for _ in range(4):
        advance(fetch)

    contract_last = (((1,), (1,)), ((), ()))
    cand_real = cands[0]
    cand_imag = cands[1]
    inner = lax.dot_general(cand_real, queries[0], contract_last, preferred_element_type=F32)
    inner = inner + lax.dot_general(cand_imag, queries[1], contract_last, preferred_element_type=F32)
    norm = jnp.sum(jnp.square(cand_real.astype(F32)), axis=1, keepdims=True)
    norm = norm + jnp.sum(jnp.square(cand_imag.astype(F32)), axis=1, keepdims=True)
    scores = (2.0 * inner - norm) / SOFTMAX_TEMPER
    top = jnp.max(scores, axis=0, keepdims=True)
    log_total = top + jnp.log(jnp.sum(jnp.exp(scores - top), axis=0, keepdims=True))
    target = lax.broadcasted_iota(jnp.int32, (n_cand, q_dev), 0) == target_pos[...]
    losses_out[...] = log_total - jnp.sum(jnp.where(target, scores, 0.0), axis=0, keepdims=True)
    weights = jnp.exp(scores - log_total) - target.astype(F32)
    weights_low = weights.astype(BF16)
    weight_sums = jnp.sum(weights, axis=1, keepdims=True)
    weights_by_query = weights.T.astype(BF16)
    scale = 2.0 / SOFTMAX_TEMPER

    def cand_part(side):
        return scale * (
            jnp.dot(weights_low, queries[side], preferred_element_type=F32)
            - weight_sums * cands[side].astype(F32)
        )

    refs = (g_acc, g_stage, grads, (g_r0, g_r1, g_r2, g_r3))
    cand_reduce = [
        Exchange(refs, low, length, i % 2, sems, place)
        for i, (low, length) in enumerate(chunks(n_cand, CHUNK))
    ]
    rel_reduce = [
        Exchange(refs, n_cand + low, length, i % 2, sems, place)
        for i, (low, length) in enumerate(chunks(rel_half, CHUNK))
    ]

    def swap(group):
        for exchange in group:
            rows = pl.ds(exchange.base, exchange.length)
            exchange.go(s_stage.at[rows, :], s_recv.at[rows, :], ent, 1 - grp)

    def merge(group):
        for exchange in group:
            exchange.land()
            rows = pl.ds(exchange.base, exchange.length)
            g_acc[rows, :] += s_recv[rows, :].astype(F32)
            exchange.advance()

    s_stage[pl.ds(0, n_cand), :] = cand_part(1 - grp).astype(BF16)
    swap(cand_reduce)
    g_acc[pl.ds(0, n_cand), :] = cand_part(grp)
    merge(cand_reduce)

    real_grad = scale * jnp.dot(weights_by_query, cand_real, preferred_element_type=F32)
    imag_grad = scale * jnp.dot(weights_by_query, cand_imag, preferred_element_type=F32)
    angle_grad = imag_grad * real_query - real_grad * imag_query
    angle_high = angle_grad.astype(BF16)
    angle_low = (angle_grad - angle_high.astype(F32)).astype(BF16)

    def rel_part(side):
        rows = lax.broadcasted_iota(jnp.int32, (rel_half, q_dev), 0) + side * rel_half
        pick = (rows == rel_ids[...]).astype(F32).astype(BF16)
        return jnp.dot(pick, angle_high, preferred_element_type=F32) + jnp.dot(
            pick, angle_low, preferred_element_type=F32
        )

    s_stage[pl.ds(n_cand, rel_half), :] = rel_part(1 - grp).astype(BF16)
    swap(rel_reduce)
    g_acc[pl.ds(n_cand, rel_half), :] = rel_part(grp)
    advance(cand_reduce)
    merge(rel_reduce)

    head_out[:, pl.ds(0, half)] = (real_grad * cosine + imag_grad * sine).astype(BF16)
    head_out[:, pl.ds(half, half)] = (imag_grad * cosine - real_grad * sine).astype(BF16)
    stores = []

    def store(src, dst):
        copy = pltpu.make_async_copy(src, dst, local_sem.at[1 + len(stores)])
        copy.start()
        stores.append(copy)

    store(head_out, head_any)
    for _ in range(6):
        advance(cand_reduce)
        advance(rel_reduce)
    block = pl.ds(0, n_cand)
    store(grads.at[:, block, :], grads_any.at[:, block, :])

    advance(rel_reduce)
    block = pl.ds(n_cand, rel_half)
    store(grads.at[:, block, :], grads_any.at[:, block, :])
    for exchange in fetch + cand_reduce + rel_reduce:
        exchange.finish()
    for copy in stores:
        copy.wait()


def finish(
    block_owner,
    block_local,
    losses_in,
    head_in,
    grads_in,
    losses_out,
    head_out,
    table_out,
    rel_out,
    losses,
    head,
    grads,
    table,
    rel,
    sem,
):
    ent = lax.axis_index("ent")
    blocks = block_owner.shape[0]
    n_cand = blocks * BLK
    rel_half = grads.shape[1] - n_cand
    half = grads.shape[2]
    begun = []

    def copy(src, dst):
        begun.append(pltpu.make_async_copy(src, dst, sem.at[len(begun)]))
        begun[-1].start()
        return begun[-1]

    cand_rows, rel_rows = pl.ds(0, n_cand), pl.ds(n_cand, rel_half)
    cand_load = copy(grads_in.at[:, cand_rows, :], grads.at[:, cand_rows, :])
    rel_load = copy(grads_in.at[:, rel_rows, :], grads.at[:, rel_rows, :])
    head_load = copy(head_in, head)
    losses_load = copy(losses_in, losses)
    stores = []
    cand_load.wait()
    for local in range(table.shape[0] // BLK):
        rows = pl.ds(local * BLK, BLK)
        for side in range(2):
            total = jnp.zeros((BLK, half), F32)
            for b in range(blocks):
                mine = jnp.logical_and(block_owner[b] == ent, block_local[b] == local)
                value = grads[side, pl.ds(b * BLK, BLK), :].astype(F32)
                total = total + jnp.where(mine, value, 0.0)
            table[rows, pl.ds(side * half, half)] = total.astype(BF16)
        stores.append(copy(table.at[rows, :], table_out.at[rows, :]))
    rel_load.wait()
    tail = rel.shape[0] - rel_half
    rel[pl.ds(0, rel_half), :] = grads[0, rel_rows, :].astype(F32)
    rel[pl.ds(rel_half, tail), :] = grads[1, rel_rows, :].astype(F32)[:tail]
    stores.append(copy(rel, rel_out))
    head_load.wait()
    stores.append(copy(head, head_out))
    losses_load.wait()
    stores.append(copy(losses, losses_out))
    for one in stores:
        one.wait()


def body(n_ent, entity_table, rel_phases, head_ids, rel_ids, target_pos, block_owner, block_local):
    rel_count, half = rel_phases.shape
    shard_rows = entity_table.shape[0]
    q_dev = head_ids.shape[0]
    n_cand = block_owner.shape[0] * BLK
    rel_half = -(-rel_count // (2 * 64)) * 64
    g_rows = n_cand + rel_half
    rest = n_ent // SPLIT
    cand_chunks, rel_chunks = len(chunks(n_cand, CHUNK)), len(chunks(rel_half, CHUNK))
    each = 2 * (1 + 1 + 3) + 1 + rest - 1
    copies = each * (2 * cand_chunks + rel_chunks) + cand_chunks + rel_chunks

    def slots(rows):
        tile = half // LINE[1]
        return [
            pltpu.VMEM((rows // 2, half), BF16),
            pltpu.VMEM((rows // 4, half), BF16),
            pltpu.VMEM((3, rows // 4, tile), BF16),
            pltpu.VMEM((max(rest - 1, 1), rows // 4, tile), BF16),
        ]

    vmem = pl.BlockSpec(memory_space=pltpu.VMEM)
    smem = pl.BlockSpec(memory_space=pltpu.SMEM)
    anywhere = pl.BlockSpec(memory_space=pl.ANY)
    losses_type = jax.ShapeDtypeStruct((1, q_dev), F32)
    head_type = jax.ShapeDtypeStruct((q_dev, 2 * half), BF16)
    raw = pl.pallas_call(
        functools.partial(kernel, n_ent),
        out_shape=(losses_type, head_type, jax.ShapeDtypeStruct((2, g_rows, half), BF16)),
        in_specs=[smem, smem, vmem, anywhere] + [vmem] * 3,
        out_specs=(vmem, anywhere, anywhere),
        scratch_shapes=[
            pltpu.VMEM((n_cand, half), F32),
            pltpu.VMEM((n_cand, half), BF16),
            pltpu.VMEM((2, n_cand, half), BF16),
            pltpu.VMEM((g_rows, half), F32),
            pltpu.VMEM((g_rows, half), BF16),
            pltpu.VMEM((2, g_rows, half), BF16),
            pltpu.VMEM((g_rows, half), BF16),
            pltpu.VMEM((g_rows, half), BF16),
            *slots(n_cand),
            *slots(g_rows),
            pltpu.VMEM((rel_count, half), F32),
            pltpu.VMEM((2 * rel_half, half), F32),
            pltpu.VMEM((2, q_dev, half), BF16),
            pltpu.VMEM((q_dev, 2 * half), BF16),
            pltpu.SemaphoreType.DMA((4,)),
            pltpu.SemaphoreType.DMA((copies,)),
            pltpu.SemaphoreType.DMA((copies,)),
        ],
        compiler_params=pltpu.CompilerParams(collective_id=0, has_side_effects=True),
    )(
        block_owner,
        block_local,
        entity_table,
        rel_phases,
        head_ids.reshape(1, q_dev),
        rel_ids.reshape(1, q_dev),
        target_pos.reshape(1, q_dev),
    )
    table_type = jax.ShapeDtypeStruct((shard_rows, 2 * half), BF16)
    rel_type = jax.ShapeDtypeStruct((rel_count, half), F32)
    losses, head_grad, table_grad, rel_grad = pl.pallas_call(
        finish,
        out_shape=(losses_type, head_type, table_type, rel_type),
        in_specs=[smem, smem] + [anywhere] * 3,
        out_specs=(anywhere,) * 4,
        scratch_shapes=[
            pltpu.VMEM((1, q_dev), F32),
            pltpu.VMEM((q_dev, 2 * half), BF16),
            pltpu.VMEM((2, g_rows, half), BF16),
            pltpu.VMEM((shard_rows, 2 * half), BF16),
            pltpu.VMEM((rel_count, half), F32),
            pltpu.SemaphoreType.DMA((7 + shard_rows // BLK,)),
        ],
    )(block_owner, block_local, *raw)
    return losses.reshape(q_dev), head_grad, table_grad, rel_grad


def solution(mesh):
    return jax.shard_map(
        functools.partial(body, mesh.shape["ent"]),
        mesh=mesh,
        in_specs=(
            P("ent", None),
            P(),
            P(("ent", "grp")),
            P(("ent", "grp")),
            P(("ent", "grp")),
            P(),
            P(),
        ),
        out_specs=(P(("ent", "grp")), P(("ent", "grp"), None), P("ent", None), P()),
        check_vma=False,
    )
```

```python
import functools

import jax
import jax.numpy as jnp
from jax import lax
from jax.experimental import pallas as pl
from jax.experimental.pallas import tpu as pltpu
from jax.sharding import PartitionSpec as P

BLK = 128
SOFTMAX_TEMPER = 2.0
MESH = pl.DeviceIdType.MESH
F32 = jnp.float32
BF16 = jnp.bfloat16
ORDERS = (((1, 2), (2, 2)), ((2, 2), (1, 2)))
LINE = (4, 4)
SPLIT = 16
CHUNK = 128


class Exchange:
    def __init__(self, refs, low, length, order, sems, place):
        self.acc, self.stage, self.out, self.slots = refs
        self.base, self.low, self.length, self.order = low, low, length, ORDERS[order]
        self.sems = sems
        self.ent, self.grp, self.rest = place
        self.wide = self.acc.shape[1] // LINE[1]
        self.started = []
        self.live = []
        self.step = 0

    def go(self, src, dst, ent, grp):
        send, recv = self.sems
        number = len(send[1])
        send[1].append(number)
        copy = pltpu.make_async_remote_copy(
            src_ref=src,
            dst_ref=dst,
            send_sem=send[0].at[number],
            recv_sem=recv.at[number],
            device_id=(ent, grp),
            device_id_type=MESH,
        )
        copy.start()
        self.started.append(copy)
        self.live.append(copy)

    def land(self):
        for copy in self.live:
            copy.wait_recv()
        self.live = []

    def rows(self, low, length):
        return pl.ds(pl.multiple_of(low, 16), length)

    def tile(self, number):
        return pl.ds(pl.multiple_of(number * self.wide, 128), self.wide)

    def coordinate(self, stride, size):
        return lax.rem(self.ent // stride, size)

    def peers(self, stride, size):
        mine = self.coordinate(stride, size)
        for k in range(1, size):
            theirs = lax.rem(mine + k, size)
            yield k - 1, theirs, self.ent + (theirs - mine) * stride

    def low_copy(self, rows):
        if self.stage is not self.acc:
            self.stage[rows, :] = self.acc[rows, :].astype(BF16)

    def scatter_start(self, p):
        stride, size = self.order[p]
        part = self.length // size
        for _, theirs, peer in self.peers(stride, size):
            rows = self.rows(self.low + theirs * part, part)
            self.low_copy(rows)
            slot = self.slots[p].at[pl.ds(self.base // (2 << p), part), :]
            self.go(self.stage.at[rows, :], slot, peer, self.grp)

    def scatter_finish(self, p):
        self.land()
        stride, size = self.order[p]
        part = self.length // size
        self.low = self.low + self.coordinate(stride, size) * part
        self.length = part
        rows = self.rows(self.low, part)
        arrived = self.slots[p][pl.ds(self.base // (2 << p), part), :].astype(F32)
        self.acc[rows, :] = (self.acc[rows, :].astype(F32) + arrived).astype(self.acc.dtype)

    def line_start(self):
        rows = self.rows(self.low, self.length)
        self.low_copy(rows)
        for k, theirs, peer in self.peers(*LINE):
            slot = self.slots[2].at[k, pl.ds(self.base // 4, self.length), :]
            self.go(self.stage.at[rows, self.tile(theirs)], slot, peer, self.grp)

    def line_finish(self):
        self.land()
        rows = self.rows(self.low, self.length)
        mine = self.tile(self.coordinate(*LINE))
        total = self.acc[rows, mine].astype(F32)
        for k in range(LINE[1] - 1):
            total = total + self.slots[2][k, pl.ds(self.base // 4, self.length), :].astype(F32)
        if self.rest > 1:
            self.stage[rows, mine] = total.astype(BF16)
            for k, _, peer in self.peers(SPLIT, self.rest):
                slot = self.slots[3].at[k, pl.ds(self.base // 4, self.length), :]
                self.go(self.stage.at[rows, mine], slot, peer, self.grp)
            self.land()
            total = self.stage[rows, mine].astype(F32)
            for k in range(self.rest - 1):
                total = total + self.slots[3][k, pl.ds(self.base // 4, self.length), :].astype(F32)
        self.out[self.grp, rows, mine] = total.astype(BF16)

    def line_gather_start(self):
        rows = self.rows(self.low, self.length)
        block = self.out.at[self.grp, rows, self.tile(self.coordinate(*LINE))]
        for _, _, peer in self.peers(*LINE):
            self.go(block, block, peer, self.grp)

    def gather_start(self, p):
        block = self.out.at[self.grp, self.rows(self.low, self.length), :]
        for _, _, peer in self.peers(*self.order[p]):
            self.go(block, block, peer, self.grp)

    def gather_finish(self, p):
        self.land()
        self.low = self.low - self.coordinate(*self.order[p]) * self.length
        self.length = self.length * self.order[p][1]

    def sibling_start(self):
        block = self.out.at[self.grp, pl.ds(self.base, self.length), :]
        self.go(block, block, self.ent, 1 - self.grp)

    def advance(self):
        if self.step == 0:
            self.scatter_start(0)
        elif self.step == 1:
            self.scatter_finish(0)
            self.scatter_start(1)
        elif self.step == 2:
            self.scatter_finish(1)
            self.line_start()
        elif self.step == 3:
            self.line_finish()
            self.line_gather_start()
        elif self.step == 4:
            self.land()
            self.gather_start(1)
        elif self.step == 5:
            self.gather_finish(1)
            self.gather_start(0)
        elif self.step == 6:
            self.gather_finish(0)
            self.sibling_start()
        elif self.step == 7:
            self.land()
        self.step += 1

    def finish(self):
        for copy in self.started:
            copy.wait_send()


def chunks(total, length):
    return [(low, min(length, total - low)) for low in range(0, total, length)]


def kernel(
    n_ent,
    block_owner,
    block_local,
    table_hbm,
    phases,
    head_ids,
    rel_ids,
    target_pos,
    losses_out,
    head_any,
    grads_any,
    c_acc,
    cands,
    g_acc,
    g_stage,
    grads,
    s_stage,
    s_recv,
    c_r0,
    c_r1,
    c_r2,
    c_r3,
    g_r0,
    g_r1,
    g_r2,
    g_r3,
    table,
    loaded,
    padded,
    queries,
    head_out,
    local_sem,
    send,
    recv,
):
    ent = lax.axis_index("ent")
    grp = lax.axis_index("grp")
    rest = n_ent // SPLIT
    half = phases.shape[1]
    rel_count = phases.shape[0]
    rel_half = padded.shape[0] // 2
    n_cand = c_acc.shape[0]
    blocks = n_cand // BLK
    q_dev = head_ids.shape[1]

    first = pltpu.make_async_copy(table_hbm, table, local_sem.at[4])
    first.start()
    load = pltpu.make_async_copy(phases, loaded, local_sem.at[0])
    load.start()
    barrier = pltpu.get_barrier_semaphore()
    partners = [(ent, 1 - grp)]
    for stride, size in ORDERS[0] + (LINE, (SPLIT, rest)):
        mine = lax.rem(ent // stride, size)
        for k in range(1, size):
            partners.append((ent + (lax.rem(mine + k, size) - mine) * stride, grp))
    for partner in partners:
        pl.semaphore_signal(barrier, inc=1, device_id=partner, device_id_type=MESH)

    my_columns = pl.ds(pl.multiple_of(grp * half, 128), half)
    first.wait()
    for b in range(blocks):
        total = jnp.zeros((BLK, half), F32)
        for local in range(table.shape[0] // BLK):
            wanted = jnp.logical_and(block_owner[b] == ent, block_local[b] == local)
            value = table[pl.ds(local * BLK, BLK), my_columns].astype(F32)
            total = jnp.where(wanted, value, total)
        c_acc[pl.ds(b * BLK, BLK), :] = total.astype(BF16)

    pl.semaphore_wait(barrier, len(partners))

    place = (ent, grp, rest)
    sems = ((send, []), recv)
    refs = (c_acc, c_acc, cands, (c_r0, c_r1, c_r2, c_r3))
    fetch = [
        Exchange(refs, low, length, i % 2, sems, place)
        for i, (low, length) in enumerate(chunks(n_cand, CHUNK))
    ]

    def advance(group):
        for exchange in group:
            exchange.advance()

    advance(fetch)

    rows_t = lax.broadcasted_iota(jnp.int32, (table.shape[0], q_dev), 0)
    head_pick = (rows_t == head_ids[...]).astype(F32).T.astype(BF16)
    heads = jnp.dot(head_pick, table[...], preferred_element_type=F32)
    rel_rows = lax.broadcasted_iota(jnp.int32, (2 * rel_half, q_dev), 0)
    rel_pick = (rel_rows == rel_ids[...]).astype(F32).T.astype(BF16)

    advance(fetch)

    load.wait()
    padded[...] = jnp.zeros_like(padded)
    padded[pl.ds(0, rel_count), :] = loaded[...]

    advance(fetch)

    whole = padded[...]
    top_part = whole.astype(BF16)
    left = whole - top_part.astype(F32)
    mid_part = left.astype(BF16)
    low_part = (left - mid_part.astype(F32)).astype(BF16)
    angles = (
        jnp.dot(rel_pick, low_part, preferred_element_type=F32)
        + jnp.dot(rel_pick, mid_part, preferred_element_type=F32)
    ) + jnp.dot(rel_pick, top_part, preferred_element_type=F32)

    advance(fetch)

    cosine = jnp.cos(angles)
    sine = jnp.sin(angles)

    advance(fetch)

    real_head = heads[:, :half]
    imag_head = heads[:, half:]
    real_query = real_head * cosine - imag_head * sine
    imag_query = real_head * sine + imag_head * cosine
    queries[0] = real_query.astype(BF16)
    queries[1] = imag_query.astype(BF16)

    for _ in range(3):
        advance(fetch)

    contract_last = (((1,), (1,)), ((), ()))
    cand_real = cands[0]
    cand_imag = cands[1]
    inner = lax.dot_general(cand_real, queries[0], contract_last, preferred_element_type=F32)
    inner = inner + lax.dot_general(cand_imag, queries[1], contract_last, preferred_element_type=F32)
    norm = jnp.sum(jnp.square(cand_real.astype(F32)), axis=1, keepdims=True)
    norm = norm + jnp.sum(jnp.square(cand_imag.astype(F32)), axis=1, keepdims=True)
    scores = (2.0 * inner - norm) / SOFTMAX_TEMPER
    top = jnp.max(scores, axis=0, keepdims=True)
    log_total = top + jnp.log(jnp.sum(jnp.exp(scores - top), axis=0, keepdims=True))
    target = lax.broadcasted_iota(jnp.int32, (n_cand, q_dev), 0) == target_pos[...]
    losses_out[...] = log_total - jnp.sum(jnp.where(target, scores, 0.0), axis=0, keepdims=True)
    weights = jnp.exp(scores - log_total) - target.astype(F32)
    weights_low = weights.astype(BF16)
    weight_sums = jnp.sum(weights, axis=1, keepdims=True)
    weights_by_query = weights.T.astype(BF16)
    scale = 2.0 / SOFTMAX_TEMPER

    def cand_part(side):
        return scale * (
            jnp.dot(weights_low, queries[side], preferred_element_type=F32)
            - weight_sums * cands[side].astype(F32)
        )

    refs = (g_acc, g_stage, grads, (g_r0, g_r1, g_r2, g_r3))
    cand_reduce = [
        Exchange(refs, low, length, i % 2, sems, place)
        for i, (low, length) in enumerate(chunks(n_cand, CHUNK))
    ]
    rel_reduce = [
        Exchange(refs, n_cand + low, length, i % 2, sems, place)
        for i, (low, length) in enumerate(chunks(rel_half, CHUNK))
    ]

    def swap(group):
        for exchange in group:
            rows = pl.ds(exchange.base, exchange.length)
            exchange.go(s_stage.at[rows, :], s_recv.at[rows, :], ent, 1 - grp)

    def merge(group):
        for exchange in group:
            exchange.land()
            rows = pl.ds(exchange.base, exchange.length)
            g_acc[rows, :] += s_recv[rows, :].astype(F32)
            exchange.advance()

    s_stage[pl.ds(0, n_cand), :] = cand_part(1 - grp).astype(BF16)
    swap(cand_reduce)
    g_acc[pl.ds(0, n_cand), :] = cand_part(grp)
    merge(cand_reduce)

    real_grad = scale * jnp.dot(weights_by_query, cand_real, preferred_element_type=F32)
    imag_grad = scale * jnp.dot(weights_by_query, cand_imag, preferred_element_type=F32)
    angle_grad = imag_grad * real_query - real_grad * imag_query
    angle_high = angle_grad.astype(BF16)
    angle_low = (angle_grad - angle_high.astype(F32)).astype(BF16)

    def rel_part(side):
        rows = lax.broadcasted_iota(jnp.int32, (rel_half, q_dev), 0) + side * rel_half
        pick = (rows == rel_ids[...]).astype(F32).astype(BF16)
        return jnp.dot(pick, angle_high, preferred_element_type=F32) + jnp.dot(
            pick, angle_low, preferred_element_type=F32
        )

    s_stage[pl.ds(n_cand, rel_half), :] = rel_part(1 - grp).astype(BF16)
    swap(rel_reduce)
    g_acc[pl.ds(n_cand, rel_half), :] = rel_part(grp)
    advance(cand_reduce)
    merge(rel_reduce)

    head_out[:, pl.ds(0, half)] = (real_grad * cosine + imag_grad * sine).astype(BF16)
    head_out[:, pl.ds(half, half)] = (imag_grad * cosine - real_grad * sine).astype(BF16)
    stores = []

    def store(src, dst):
        copy = pltpu.make_async_copy(src, dst, local_sem.at[1 + len(stores)])
        copy.start()
        stores.append(copy)

    store(head_out, head_any)
    for _ in range(6):
        advance(cand_reduce)
        advance(rel_reduce)
    block = pl.ds(0, n_cand)
    store(grads.at[:, block, :], grads_any.at[:, block, :])

    advance(rel_reduce)
    block = pl.ds(n_cand, rel_half)
    store(grads.at[:, block, :], grads_any.at[:, block, :])
    for exchange in fetch + cand_reduce + rel_reduce:
        exchange.finish()
    for copy in stores:
        copy.wait()


def finish(
    block_owner,
    block_local,
    losses_in,
    head_in,
    grads_in,
    losses_out,
    head_out,
    table_out,
    rel_out,
    losses,
    head,
    grads,
    table,
    rel,
    sem,
):
    ent = lax.axis_index("ent")
    blocks = block_owner.shape[0]
    n_cand = blocks * BLK
    rel_half = grads.shape[1] - n_cand
    half = grads.shape[2]
    begun = []

    def copy(src, dst):
        begun.append(pltpu.make_async_copy(src, dst, sem.at[len(begun)]))
        begun[-1].start()
        return begun[-1]

    cand_rows, rel_rows = pl.ds(0, n_cand), pl.ds(n_cand, rel_half)
    cand_load = copy(grads_in.at[:, cand_rows, :], grads.at[:, cand_rows, :])
    rel_load = copy(grads_in.at[:, rel_rows, :], grads.at[:, rel_rows, :])
    head_load = copy(head_in, head)
    losses_load = copy(losses_in, losses)
    stores = []
    cand_load.wait()
    for local in range(table.shape[0] // BLK):
        rows = pl.ds(local * BLK, BLK)
        for side in range(2):
            total = jnp.zeros((BLK, half), F32)
            for b in range(blocks):
                mine = jnp.logical_and(block_owner[b] == ent, block_local[b] == local)
                value = grads[side, pl.ds(b * BLK, BLK), :].astype(F32)
                total = total + jnp.where(mine, value, 0.0)
            table[rows, pl.ds(side * half, half)] = total.astype(BF16)
        stores.append(copy(table.at[rows, :], table_out.at[rows, :]))
    rel_load.wait()
    tail = rel.shape[0] - rel_half
    rel[pl.ds(0, rel_half), :] = grads[0, rel_rows, :].astype(F32)
    rel[pl.ds(rel_half, tail), :] = grads[1, rel_rows, :].astype(F32)[:tail]
    stores.append(copy(rel, rel_out))
    head_load.wait()
    stores.append(copy(head, head_out))
    losses_load.wait()
    stores.append(copy(losses, losses_out))
    for one in stores:
        one.wait()


def body(n_ent, entity_table, rel_phases, head_ids, rel_ids, target_pos, block_owner, block_local):
    rel_count, half = rel_phases.shape
    shard_rows = entity_table.shape[0]
    q_dev = head_ids.shape[0]
    n_cand = block_owner.shape[0] * BLK
    rel_half = -(-rel_count // (2 * 64)) * 64
    g_rows = n_cand + rel_half
    rest = n_ent // SPLIT
    cand_chunks, rel_chunks = len(chunks(n_cand, CHUNK)), len(chunks(rel_half, CHUNK))
    each = 2 * (1 + 1 + 3) + 1 + rest - 1
    copies = each * (2 * cand_chunks + rel_chunks) + cand_chunks + rel_chunks

    def slots(rows):
        tile = half // LINE[1]
        return [
            pltpu.VMEM((rows // 2, half), BF16),
            pltpu.VMEM((rows // 4, half), BF16),
            pltpu.VMEM((3, rows // 4, tile), BF16),
            pltpu.VMEM((max(rest - 1, 1), rows // 4, tile), BF16),
        ]

    vmem = pl.BlockSpec(memory_space=pltpu.VMEM)
    smem = pl.BlockSpec(memory_space=pltpu.SMEM)
    anywhere = pl.BlockSpec(memory_space=pl.ANY)
    hbm = pl.BlockSpec(memory_space=pltpu.HBM)
    losses_type = jax.ShapeDtypeStruct((1, q_dev), F32)
    head_type = jax.ShapeDtypeStruct((q_dev, 2 * half), BF16)
    raw = pl.pallas_call(
        functools.partial(kernel, n_ent),
        out_shape=(losses_type, head_type, jax.ShapeDtypeStruct((2, g_rows, half), BF16)),
        in_specs=[smem, smem, hbm, hbm] + [vmem] * 3,
        out_specs=(vmem, anywhere, anywhere),
        scratch_shapes=[
            pltpu.VMEM((n_cand, half), BF16),
            pltpu.VMEM((2, n_cand, half), BF16),
            pltpu.VMEM((g_rows, half), F32),
            pltpu.VMEM((g_rows, half), BF16),
            pltpu.VMEM((2, g_rows, half), BF16),
            pltpu.VMEM((g_rows, half), BF16),
            pltpu.VMEM((g_rows, half), BF16),
            *slots(n_cand),
            *slots(g_rows),
            pltpu.VMEM((shard_rows, 2 * half), BF16),
            pltpu.VMEM((rel_count, half), F32),
            pltpu.VMEM((2 * rel_half, half), F32),
            pltpu.VMEM((2, q_dev, half), BF16),
            pltpu.VMEM((q_dev, 2 * half), BF16),
            pltpu.SemaphoreType.DMA((5,)),
            pltpu.SemaphoreType.DMA((copies,)),
            pltpu.SemaphoreType.DMA((copies,)),
        ],
        compiler_params=pltpu.CompilerParams(collective_id=0, has_side_effects=True),
    )(
        block_owner,
        block_local,
        entity_table,
        rel_phases,
        head_ids.reshape(1, q_dev),
        rel_ids.reshape(1, q_dev),
        target_pos.reshape(1, q_dev),
    )
    table_type = jax.ShapeDtypeStruct((shard_rows, 2 * half), BF16)
    rel_type = jax.ShapeDtypeStruct((rel_count, half), F32)
    losses, head_grad, table_grad, rel_grad = pl.pallas_call(
        finish,
        out_shape=(losses_type, head_type, table_type, rel_type),
        in_specs=[smem, smem] + [anywhere] * 3,
        out_specs=(anywhere,) * 4,
        scratch_shapes=[
            pltpu.VMEM((1, q_dev), F32),
            pltpu.VMEM((q_dev, 2 * half), BF16),
            pltpu.VMEM((2, g_rows, half), BF16),
            pltpu.VMEM((shard_rows, 2 * half), BF16),
            pltpu.VMEM((rel_count, half), F32),
            pltpu.SemaphoreType.DMA((7 + shard_rows // BLK,)),
        ],
    )(block_owner, block_local, *raw)
    return losses.reshape(q_dev), head_grad, table_grad, rel_grad


def solution(mesh):
    return jax.shard_map(
        functools.partial(body, mesh.shape["ent"]),
        mesh=mesh,
        in_specs=(
            P("ent", None),
            P(),
            P(("ent", "grp")),
            P(("ent", "grp")),
            P(("ent", "grp")),
            P(),
            P(),
        ),
        out_specs=(P(("ent", "grp")), P(("ent", "grp"), None), P("ent", None), P()),
        check_vma=False,
    )
```

```python
import functools

import jax
import jax.numpy as jnp
from jax import lax
from jax.experimental import pallas as pl
from jax.experimental.pallas import tpu as pltpu
from jax.sharding import PartitionSpec as P

BLK = 128
SOFTMAX_TEMPER = 2.0
MESH = pl.DeviceIdType.MESH
F32 = jnp.float32
BF16 = jnp.bfloat16
ORDERS = (((1, 2), (2, 2)), ((2, 2), (1, 2)))
LINE = (4, 4)
SPLIT = 16
CHUNK = 128


class Exchange:
    def __init__(self, refs, low, length, order, sems, place):
        self.acc, self.stage, self.out, self.slots = refs
        self.base, self.low, self.length, self.order = low, low, length, ORDERS[order]
        self.sems = sems
        self.ent, self.grp, self.rest = place
        self.wide = self.acc.shape[1] // LINE[1]
        self.started = []
        self.live = []
        self.step = 0

    def go(self, src, dst, ent, grp):
        send, recv = self.sems
        number = len(send[1])
        send[1].append(number)
        copy = pltpu.make_async_remote_copy(
            src_ref=src,
            dst_ref=dst,
            send_sem=send[0].at[number],
            recv_sem=recv.at[number],
            device_id=(ent, grp),
            device_id_type=MESH,
        )
        copy.start()
        self.started.append(copy)
        self.live.append(copy)

    def land(self):
        for copy in self.live:
            copy.wait_recv()
        self.live = []

    def rows(self, low, length):
        return pl.ds(pl.multiple_of(low, 16), length)

    def tile(self, number):
        return pl.ds(pl.multiple_of(number * self.wide, 128), self.wide)

    def coordinate(self, stride, size):
        return lax.rem(self.ent // stride, size)

    def peers(self, stride, size):
        mine = self.coordinate(stride, size)
        for k in range(1, size):
            theirs = lax.rem(mine + k, size)
            yield k - 1, theirs, self.ent + (theirs - mine) * stride

    def low_copy(self, rows):
        if self.stage is not self.acc:
            self.stage[rows, :] = self.acc[rows, :].astype(BF16)

    def scatter_start(self, p):
        stride, size = self.order[p]
        part = self.length // size
        for _, theirs, peer in self.peers(stride, size):
            rows = self.rows(self.low + theirs * part, part)
            self.low_copy(rows)
            slot = self.slots[p].at[pl.ds(self.base // (2 << p), part), :]
            self.go(self.stage.at[rows, :], slot, peer, self.grp)

    def scatter_finish(self, p):
        self.land()
        stride, size = self.order[p]
        part = self.length // size
        self.low = self.low + self.coordinate(stride, size) * part
        self.length = part
        rows = self.rows(self.low, part)
        arrived = self.slots[p][pl.ds(self.base // (2 << p), part), :].astype(F32)
        self.acc[rows, :] = (self.acc[rows, :].astype(F32) + arrived).astype(self.acc.dtype)

    def line_start(self):
        rows = self.rows(self.low, self.length)
        self.low_copy(rows)
        for k, theirs, peer in self.peers(*LINE):
            slot = self.slots[2].at[k, pl.ds(self.base // 4, self.length), :]
            self.go(self.stage.at[rows, self.tile(theirs)], slot, peer, self.grp)

    def line_finish(self):
        self.land()
        rows = self.rows(self.low, self.length)
        mine = self.tile(self.coordinate(*LINE))
        total = self.acc[rows, mine].astype(F32)
        for k in range(LINE[1] - 1):
            total = total + self.slots[2][k, pl.ds(self.base // 4, self.length), :].astype(F32)
        if self.rest > 1:
            self.stage[rows, mine] = total.astype(BF16)
            for k, _, peer in self.peers(SPLIT, self.rest):
                slot = self.slots[3].at[k, pl.ds(self.base // 4, self.length), :]
                self.go(self.stage.at[rows, mine], slot, peer, self.grp)
            self.land()
            total = self.stage[rows, mine].astype(F32)
            for k in range(self.rest - 1):
                total = total + self.slots[3][k, pl.ds(self.base // 4, self.length), :].astype(F32)
        self.out[self.grp, rows, mine] = total.astype(BF16)

    def line_gather_start(self):
        rows = self.rows(self.low, self.length)
        block = self.out.at[self.grp, rows, self.tile(self.coordinate(*LINE))]
        for _, _, peer in self.peers(*LINE):
            self.go(block, block, peer, self.grp)

    def gather_start(self, p):
        block = self.out.at[self.grp, self.rows(self.low, self.length), :]
        for _, _, peer in self.peers(*self.order[p]):
            self.go(block, block, peer, self.grp)

    def gather_finish(self, p):
        self.land()
        self.low = self.low - self.coordinate(*self.order[p]) * self.length
        self.length = self.length * self.order[p][1]

    def sibling_start(self):
        block = self.out.at[self.grp, pl.ds(self.base, self.length), :]
        self.go(block, block, self.ent, 1 - self.grp)

    def advance(self):
        if self.step == 0:
            self.scatter_start(0)
        elif self.step == 1:
            self.scatter_finish(0)
            self.scatter_start(1)
        elif self.step == 2:
            self.scatter_finish(1)
            self.line_start()
        elif self.step == 3:
            self.line_finish()
            self.line_gather_start()
        elif self.step == 4:
            self.land()
            self.gather_start(1)
        elif self.step == 5:
            self.gather_finish(1)
            self.gather_start(0)
        elif self.step == 6:
            self.gather_finish(0)
            self.sibling_start()
        elif self.step == 7:
            self.land()
        self.step += 1

    def finish(self):
        for copy in self.started:
            copy.wait_send()


def chunks(total, length):
    return [(low, min(length, total - low)) for low in range(0, total, length)]


def kernel(
    n_ent,
    block_owner,
    block_local,
    table_hbm,
    phases,
    head_ids,
    rel_ids,
    target_pos,
    losses_out,
    head_any,
    grads_any,
    c_acc,
    cands,
    g_acc,
    g_stage,
    grads,
    s_stage,
    s_recv,
    c_r0,
    c_r1,
    c_r2,
    c_r3,
    g_r0,
    g_r1,
    g_r2,
    g_r3,
    table,
    loaded,
    padded,
    queries,
    head_out,
    local_sem,
    send,
    recv,
):
    ent = lax.axis_index("ent")
    grp = lax.axis_index("grp")
    rest = n_ent // SPLIT
    half = phases.shape[1]
    rel_count = phases.shape[0]
    rel_half = padded.shape[0] // 2
    n_cand = c_acc.shape[0]
    blocks = n_cand // BLK
    q_dev = head_ids.shape[1]

    first = pltpu.make_async_copy(table_hbm, table, local_sem.at[5])
    first.start()
    load = pltpu.make_async_copy(phases, loaded, local_sem.at[0])
    load.start()
    barrier = pltpu.get_barrier_semaphore()
    partners = [(ent, 1 - grp)]
    for stride, size in ORDERS[0] + (LINE, (SPLIT, rest)):
        mine = lax.rem(ent // stride, size)
        for k in range(1, size):
            partners.append((ent + (lax.rem(mine + k, size) - mine) * stride, grp))
    for partner in partners:
        pl.semaphore_signal(barrier, inc=1, device_id=partner, device_id_type=MESH)

    my_columns = pl.ds(pl.multiple_of(grp * half, 128), half)
    first.wait()
    for b in range(blocks):
        total = jnp.zeros((BLK, half), F32)
        for local in range(table.shape[0] // BLK):
            wanted = jnp.logical_and(block_owner[b] == ent, block_local[b] == local)
            value = table[pl.ds(local * BLK, BLK), my_columns].astype(F32)
            total = jnp.where(wanted, value, total)
        c_acc[pl.ds(b * BLK, BLK), :] = total.astype(BF16)

    pl.semaphore_wait(barrier, len(partners))

    place = (ent, grp, rest)
    sems = ((send, []), recv)
    refs = (c_acc, c_acc, cands, (c_r0, c_r1, c_r2, c_r3))
    fetch = [
        Exchange(refs, low, length, i % 2, sems, place)
        for i, (low, length) in enumerate(chunks(n_cand, CHUNK))
    ]

    def advance(group):
        for exchange in group:
            exchange.advance()

    advance(fetch)

    rows_t = lax.broadcasted_iota(jnp.int32, (table.shape[0], q_dev), 0)
    head_pick = (rows_t == head_ids[...]).astype(F32).T.astype(BF16)
    heads = jnp.dot(head_pick, table[...], preferred_element_type=F32)
    rel_rows = lax.broadcasted_iota(jnp.int32, (2 * rel_half, q_dev), 0)
    rel_pick = (rel_rows == rel_ids[...]).astype(F32).T.astype(BF16)

    advance(fetch)

    load.wait()
    padded[...] = jnp.zeros_like(padded)
    padded[pl.ds(0, rel_count), :] = loaded[...]

    advance(fetch)

    whole = padded[...]
    top_part = whole.astype(BF16)
    left = whole - top_part.astype(F32)
    mid_part = left.astype(BF16)
    low_part = (left - mid_part.astype(F32)).astype(BF16)
    angles = (
        jnp.dot(rel_pick, low_part, preferred_element_type=F32)
        + jnp.dot(rel_pick, mid_part, preferred_element_type=F32)
    ) + jnp.dot(rel_pick, top_part, preferred_element_type=F32)

    advance(fetch)

    cosine = jnp.cos(angles)
    sine = jnp.sin(angles)

    advance(fetch)

    real_head = heads[:, :half]
    imag_head = heads[:, half:]
    real_query = real_head * cosine - imag_head * sine
    imag_query = real_head * sine + imag_head * cosine
    queries[0] = real_query.astype(BF16)
    queries[1] = imag_query.astype(BF16)

    for _ in range(3):
        advance(fetch)

    contract_last = (((1,), (1,)), ((), ()))
    cand_real = cands[0]
    cand_imag = cands[1]
    inner = lax.dot_general(cand_real, queries[0], contract_last, preferred_element_type=F32)
    inner = inner + lax.dot_general(cand_imag, queries[1], contract_last, preferred_element_type=F32)
    norm = jnp.sum(jnp.square(cand_real.astype(F32)), axis=1, keepdims=True)
    norm = norm + jnp.sum(jnp.square(cand_imag.astype(F32)), axis=1, keepdims=True)
    scores = (2.0 * inner - norm) / SOFTMAX_TEMPER
    top = jnp.max(scores, axis=0, keepdims=True)
    log_total = top + jnp.log(jnp.sum(jnp.exp(scores - top), axis=0, keepdims=True))
    target = lax.broadcasted_iota(jnp.int32, (n_cand, q_dev), 0) == target_pos[...]
    losses_out[...] = log_total - jnp.sum(jnp.where(target, scores, 0.0), axis=0, keepdims=True)
    weights = jnp.exp(scores - log_total) - target.astype(F32)
    weights_low = weights.astype(BF16)
    weight_sums = jnp.sum(weights, axis=1, keepdims=True)
    weights_by_query = weights.T.astype(BF16)
    scale = 2.0 / SOFTMAX_TEMPER

    def cand_part(side):
        return scale * (
            jnp.dot(weights_low, queries[side], preferred_element_type=F32)
            - weight_sums * cands[side].astype(F32)
        )

    refs = (g_acc, g_stage, grads, (g_r0, g_r1, g_r2, g_r3))
    cand_reduce = [
        Exchange(refs, low, length, i % 2, sems, place)
        for i, (low, length) in enumerate(chunks(n_cand, CHUNK))
    ]
    rel_reduce = [
        Exchange(refs, n_cand + low, length, i % 2, sems, place)
        for i, (low, length) in enumerate(chunks(rel_half, CHUNK))
    ]

    def swap(group):
        for exchange in group:
            rows = pl.ds(exchange.base, exchange.length)
            exchange.go(s_stage.at[rows, :], s_recv.at[rows, :], ent, 1 - grp)

    def merge(group):
        for exchange in group:
            exchange.land()
            rows = pl.ds(exchange.base, exchange.length)
            g_acc[rows, :] += s_recv[rows, :].astype(F32)
            exchange.advance()

    s_stage[pl.ds(0, n_cand), :] = cand_part(1 - grp).astype(BF16)
    swap(cand_reduce)
    g_acc[pl.ds(0, n_cand), :] = cand_part(grp)
    merge(cand_reduce)

    real_grad = scale * jnp.dot(weights_by_query, cand_real, preferred_element_type=F32)
    imag_grad = scale * jnp.dot(weights_by_query, cand_imag, preferred_element_type=F32)
    angle_grad = imag_grad * real_query - real_grad * imag_query
    angle_high = angle_grad.astype(BF16)
    angle_low = (angle_grad - angle_high.astype(F32)).astype(BF16)

    def rel_part(side):
        rows = lax.broadcasted_iota(jnp.int32, (rel_half, q_dev), 0) + side * rel_half
        pick = (rows == rel_ids[...]).astype(F32).astype(BF16)
        return jnp.dot(pick, angle_high, preferred_element_type=F32) + jnp.dot(
            pick, angle_low, preferred_element_type=F32
        )

    s_stage[pl.ds(n_cand, rel_half), :] = rel_part(1 - grp).astype(BF16)
    swap(rel_reduce)
    g_acc[pl.ds(n_cand, rel_half), :] = rel_part(grp)
    advance(cand_reduce)
    merge(rel_reduce)

    head_out[:, pl.ds(0, half)] = (real_grad * cosine + imag_grad * sine).astype(BF16)
    head_out[:, pl.ds(half, half)] = (imag_grad * cosine - real_grad * sine).astype(BF16)
    stores = []

    def store(src, dst):
        copy = pltpu.make_async_copy(src, dst, local_sem.at[1 + len(stores)])
        copy.start()
        stores.append(copy)

    store(head_out, head_any)
    for _ in range(6):
        advance(cand_reduce)
        advance(rel_reduce)
    block = pl.ds(0, n_cand)
    store(grads.at[:, block, :], grads_any.at[:, block, :])

    block = pl.ds(n_cand, rel_half)
    store(grads.at[grp, block, :], grads_any.at[grp, block, :])
    advance(rel_reduce)
    store(grads.at[1 - grp, block, :], grads_any.at[1 - grp, block, :])
    for exchange in fetch + cand_reduce + rel_reduce:
        exchange.finish()
    for copy in stores:
        copy.wait()


def finish(
    block_owner,
    block_local,
    losses_in,
    head_in,
    grads_in,
    losses_out,
    head_out,
    table_out,
    rel_out,
    losses,
    head,
    grads,
    table,
    rel,
    sem,
):
    ent = lax.axis_index("ent")
    blocks = block_owner.shape[0]
    n_cand = blocks * BLK
    rel_half = grads.shape[1] - n_cand
    half = grads.shape[2]
    begun = []

    def copy(src, dst):
        begun.append(pltpu.make_async_copy(src, dst, sem.at[len(begun)]))
        begun[-1].start()
        return begun[-1]

    cand_rows, rel_rows = pl.ds(0, n_cand), pl.ds(n_cand, rel_half)
    cand_load = copy(grads_in.at[:, cand_rows, :], grads.at[:, cand_rows, :])
    rel_load = copy(grads_in.at[:, rel_rows, :], grads.at[:, rel_rows, :])
    head_load = copy(head_in, head)
    losses_load = copy(losses_in, losses)
    stores = []
    cand_load.wait()
    for local in range(table.shape[0] // BLK):
        rows = pl.ds(local * BLK, BLK)
        for side in range(2):
            total = jnp.zeros((BLK, half), F32)
            for b in range(blocks):
                mine = jnp.logical_and(block_owner[b] == ent, block_local[b] == local)
                value = grads[side, pl.ds(b * BLK, BLK), :].astype(F32)
                total = total + jnp.where(mine, value, 0.0)
            table[rows, pl.ds(side * half, half)] = total.astype(BF16)
        stores.append(copy(table.at[rows, :], table_out.at[rows, :]))
    rel_load.wait()
    tail = rel.shape[0] - rel_half
    rel[pl.ds(0, rel_half), :] = grads[0, rel_rows, :].astype(F32)
    rel[pl.ds(rel_half, tail), :] = grads[1, rel_rows, :].astype(F32)[:tail]
    stores.append(copy(rel, rel_out))
    head_load.wait()
    stores.append(copy(head, head_out))
    losses_load.wait()
    stores.append(copy(losses, losses_out))
    for one in stores:
        one.wait()


def body(n_ent, entity_table, rel_phases, head_ids, rel_ids, target_pos, block_owner, block_local):
    rel_count, half = rel_phases.shape
    shard_rows = entity_table.shape[0]
    q_dev = head_ids.shape[0]
    n_cand = block_owner.shape[0] * BLK
    rel_half = -(-rel_count // (2 * 64)) * 64
    g_rows = n_cand + rel_half
    rest = n_ent // SPLIT
    cand_chunks, rel_chunks = len(chunks(n_cand, CHUNK)), len(chunks(rel_half, CHUNK))
    each = 2 * (1 + 1 + 3) + 1 + rest - 1
    copies = each * (2 * cand_chunks + rel_chunks) + cand_chunks + rel_chunks

    def slots(rows):
        tile = half // LINE[1]
        return [
            pltpu.VMEM((rows // 2, half), BF16),
            pltpu.VMEM((rows // 4, half), BF16),
            pltpu.VMEM((3, rows // 4, tile), BF16),
            pltpu.VMEM((max(rest - 1, 1), rows // 4, tile), BF16),
        ]

    vmem = pl.BlockSpec(memory_space=pltpu.VMEM)
    smem = pl.BlockSpec(memory_space=pltpu.SMEM)
    anywhere = pl.BlockSpec(memory_space=pl.ANY)
    hbm = pl.BlockSpec(memory_space=pltpu.HBM)
    losses_type = jax.ShapeDtypeStruct((1, q_dev), F32)
    head_type = jax.ShapeDtypeStruct((q_dev, 2 * half), BF16)
    raw = pl.pallas_call(
        functools.partial(kernel, n_ent),
        out_shape=(losses_type, head_type, jax.ShapeDtypeStruct((2, g_rows, half), BF16)),
        in_specs=[smem, smem, hbm, hbm] + [vmem] * 3,
        out_specs=(vmem, anywhere, anywhere),
        scratch_shapes=[
            pltpu.VMEM((n_cand, half), BF16),
            pltpu.VMEM((2, n_cand, half), BF16),
            pltpu.VMEM((g_rows, half), F32),
            pltpu.VMEM((g_rows, half), BF16),
            pltpu.VMEM((2, g_rows, half), BF16),
            pltpu.VMEM((g_rows, half), BF16),
            pltpu.VMEM((g_rows, half), BF16),
            *slots(n_cand),
            *slots(g_rows),
            pltpu.VMEM((shard_rows, 2 * half), BF16),
            pltpu.VMEM((rel_count, half), F32),
            pltpu.VMEM((2 * rel_half, half), F32),
            pltpu.VMEM((2, q_dev, half), BF16),
            pltpu.VMEM((q_dev, 2 * half), BF16),
            pltpu.SemaphoreType.DMA((6,)),
            pltpu.SemaphoreType.DMA((copies,)),
            pltpu.SemaphoreType.DMA((copies,)),
        ],
        compiler_params=pltpu.CompilerParams(collective_id=0, has_side_effects=True),
    )(
        block_owner,
        block_local,
        entity_table,
        rel_phases,
        head_ids.reshape(1, q_dev),
        rel_ids.reshape(1, q_dev),
        target_pos.reshape(1, q_dev),
    )
    table_type = jax.ShapeDtypeStruct((shard_rows, 2 * half), BF16)
    rel_type = jax.ShapeDtypeStruct((rel_count, half), F32)
    losses, head_grad, table_grad, rel_grad = pl.pallas_call(
        finish,
        out_shape=(losses_type, head_type, table_type, rel_type),
        in_specs=[smem, smem] + [anywhere] * 3,
        out_specs=(anywhere,) * 4,
        scratch_shapes=[
            pltpu.VMEM((1, q_dev), F32),
            pltpu.VMEM((q_dev, 2 * half), BF16),
            pltpu.VMEM((2, g_rows, half), BF16),
            pltpu.VMEM((shard_rows, 2 * half), BF16),
            pltpu.VMEM((rel_count, half), F32),
            pltpu.SemaphoreType.DMA((7 + shard_rows // BLK,)),
        ],
    )(block_owner, block_local, *raw)
    return losses.reshape(q_dev), head_grad, table_grad, rel_grad


def solution(mesh):
    return jax.shard_map(
        functools.partial(body, mesh.shape["ent"]),
        mesh=mesh,
        in_specs=(
            P("ent", None),
            P(),
            P(("ent", "grp")),
            P(("ent", "grp")),
            P(("ent", "grp")),
            P(),
            P(),
        ),
        out_specs=(P(("ent", "grp")), P(("ent", "grp"), None), P("ent", None), P()),
        check_vma=False,
    )
```
